32 devices in a mesh: groups: 2 (over x), seq: 16 (over z, y, core).
Axes of the slice: x: 2, y: 2, z: 4, core: 2. Of those that a mesh axis runs over, the one named last changes fastest.
Arguments:
- queries: bfloat16 [1024, 2048], P(('groups', 'seq')), parts along dimension 0, may hold values from -132 to 132
- fresh_keys: bfloat16 [1024, 2048], P(('groups', 'seq')), parts along dimension 0, may hold values from -6 to 6
- fresh_values: bfloat16 [1024, 2048], P(('groups', 'seq')), parts along dimension 0, may hold values from -48 to 48
- stale_keys: bfloat16 [1024, 2048], P(('groups', 'seq')), parts along dimension 0, may hold values from -6 to 6
- stale_values: bfloat16 [1024, 2048], P(('groups', 'seq')), parts along dimension 0, may hold values from -48 to 48
- patch_sizes: int32 [8], P('groups'), parts along dimension 0, may hold values from 1 to 256, 512 in all
Outputs:
- attended: bfloat16 [1024, 2048], P(('groups', 'seq')), parts along dimension 0
The draws below stay inside these ranges and needn't reach their ends.
There are 2 independent parts, one for each index of `groups`. The reference program is written for one: setup_inputs(seed, part) draws one part's arguments, and reference() takes and returns one part's arrays. A program takes and returns all parts, laid end to end along the dimension named above; each array names one. Nothing has to cross between parts.
Inputs may be any that keep to these rules, and one draw needn't show every extreme that they name: `patch_sizes`: the patch lengths sum to 512.
All inputs are finite; a program needn't handle non-finite values.
Results may differ from the reference program's by a relative error of at most 0.006.
Values may be sent and summed in bfloat16 or wider, within the bound.
A program may use at most 64 MiB of HBM per device.

```python
import math
import jax
import jax.numpy as jnp
import numpy as np
from jax import lax

H = 16
HD = 128
PATCHES = 4
TOKENS = 512


def base_keys(key):
    return jnp.clip(jax.random.normal(jax.random.fold_in(key, 5), (TOKENS, H * HD), jnp.float32), -6.0, 6.0)


def draw_fresh_keys(key, part):
    return base_keys(key).astype(jnp.bfloat16)


def draw_queries(key, part):
    drawn = jnp.clip(2.0 * jax.random.normal(jax.random.fold_in(key, 6), (TOKENS, H * HD), jnp.float32), -12.0, 12.0)
    return drawn.astype(jnp.bfloat16)


def block_levels(stream_key, shape, cuts, least, high):
    level = 1.0
    for axis_at, shards_of in cuts:
        steps = jax.random.uniform(jax.random.fold_in(jax.random.fold_in(stream_key, 6), axis_at), (shards_of,), jnp.float32, least / len(cuts), high / len(cuts))
        level = level * jnp.repeat(jnp.exp(steps), shape[axis_at] // shards_of).reshape((-1,) + (1,) * (len(shape) - 1 - axis_at))
    return level


def profile(number_of, total, limit, lean):
    loads = [(1 << 20) // math.isqrt(rank ** lean) + 1 for rank in range(2, number_of + 1)]
    spare, holding = total - limit - (number_of - 1), [1] * (number_of - 1)
    while spare > 0:
        free = [i for i in range(number_of - 1) if holding[i] < limit]
        mass, remaining = sum([loads[i] for i in free]), spare
        for i in free:
            more = min(limit - holding[i], max(1, remaining * loads[i] // mass), spare)
            holding[i] = holding[i] + more
            spare = spare - more
    return np.array([limit] + holding)


def ragged_sizes(rng, number_of, total, most, slope):
    if number_of == 2:
        one = jax.random.randint(rng, (), max(1, total - most), min(most, total - 1) + 1)
        return jnp.stack([one, total - one])
    sizes = jnp.asarray(profile(number_of, total, most, slope), jnp.int32)
    couples = (number_of - 1) // 2
    source_of, receiver = sizes[1:1 + 2 * couples:2], sizes[2:2 + 2 * couples:2]
    room = jnp.minimum(source_of - 1, most - receiver)
    moved = jax.random.randint(jax.random.fold_in(rng, 1), (couples,), 0, 1 << 20) % (room + 1)
    sizes = sizes.at[1:1 + 2 * couples:2].set(source_of - moved).at[2:2 + 2 * couples:2].set(receiver + moved)
    return sizes[jax.random.permutation(jax.random.fold_in(rng, 2), number_of)]


def scatter_about(own_key, extent, spread, bound, split=(), held_as=jnp.bfloat16):
    entries = jax.random.normal(own_key, extent, jnp.float32) * spread
    if len(split) > 0:
        entries = block_levels(own_key, extent, split, -0.22, 0.18) * entries
    return jnp.clip(entries, min=-bound, max=bound).astype(held_as)


def setup_inputs(seed: int = 0, part: int = 0) -> dict:
    arg_keys = jax.random.split(jax.random.key(seed), 7)
    part_keys = jax.random.split(jax.random.fold_in(arg_keys[6], part), 7)
    queries = draw_queries(jax.random.fold_in(jax.random.fold_in(arg_keys[6], part), 71), part)
    fresh_keys = draw_fresh_keys(jax.random.fold_in(jax.random.fold_in(arg_keys[6], part), 71), part)
    fresh_values = scatter_about(part_keys[2], (TOKENS, H * HD), 8.0, 48.0, ((0, 16),))
    stale_keys = scatter_about(part_keys[3], (TOKENS, H * HD), 1.0, 6.0, ((0, 16),))
    stale_values = scatter_about(part_keys[4], (TOKENS, H * HD), 8.0, 48.0, ((0, 16),))
    patch_sizes = ragged_sizes(part_keys[5], PATCHES, TOKENS, TOKENS // 2, 1).astype(jnp.int32)
    return dict(queries=queries, fresh_keys=fresh_keys, fresh_values=fresh_values, stale_keys=stale_keys, stale_values=stale_values, patch_sizes=patch_sizes)


def reference(queries, fresh_keys, fresh_values, stale_keys, stale_values, patch_sizes):
    total_rows, columns = queries.shape
    head_size = columns // H
    block_rows = math.gcd(total_rows, 512)
    patch_ends = jnp.cumsum(patch_sizes)[:-1]
    positions = jnp.arange(total_rows, dtype=jnp.int32)
    token_patch = jnp.sum((positions[:, None] >= patch_ends[None, :]).astype(jnp.int32), axis=1)
    score_scale = head_size ** -0.5

    def one_head(head):
        start = (head * head_size).astype(jnp.int32)

        def take(array):
            return lax.dynamic_slice_in_dim(array, start, head_size, 1)

        query_head = take(queries).reshape(-1, block_rows, head_size)
        key_fresh = take(fresh_keys)
        value_fresh = take(fresh_values)
        key_stale = take(stale_keys)
        value_stale = take(stale_values)
        patch_blocks = token_patch.reshape(-1, block_rows)

        def one_block(pair):
            query_block, query_patch = pair
            is_fresh = token_patch[None, :] <= query_patch[:, None]
            fresh_scores = jnp.dot(query_block, key_fresh.T, preferred_element_type=jnp.float32)
            stale_scores = jnp.dot(query_block, key_stale.T, preferred_element_type=jnp.float32)
            scores = jnp.where(is_fresh, fresh_scores, stale_scores) * score_scale
            weights = jnp.exp(scores - jnp.max(scores, axis=1, keepdims=True))
            denominator = jnp.sum(weights, axis=1, keepdims=True)
            rounded = weights.astype(jnp.bfloat16)
            zeroes = jnp.zeros_like(rounded)
            numerator = jnp.dot(jnp.where(is_fresh, rounded, zeroes), value_fresh, preferred_element_type=jnp.float32)
            numerator = numerator + jnp.dot(jnp.where(is_fresh, zeroes, rounded), value_stale, preferred_element_type=jnp.float32)
            return (numerator / denominator).astype(jnp.bfloat16)

        return lax.map(one_block, (query_head, patch_blocks)).reshape(total_rows, head_size)

    heads_out = lax.map(one_head, jnp.arange(H, dtype=jnp.int32))
    return jnp.transpose(heads_out, (1, 0, 2)).reshape(total_rows, columns)
```

```python
import functools

import jax
import jax.numpy as jnp
from jax import lax
from jax.experimental import pallas as pl
from jax.experimental.pallas import tpu as pltpu
from jax.sharding import PartitionSpec as P

H = 16
MESH = pl.DeviceIdType.MESH


def each(count, body):
    if count <= 32:
        for k in range(1, count):
            body(k)
    else:
        lax.fori_loop(1, count, lambda k, c: (body(k), c)[1], 0)


def flipped(me, k, count):
    if count & (count - 1):
        return lax.rem(me + k, count)
    peer, bit = 0, 1
    while bit < count:
        peer = peer + bit * lax.rem(me // bit + k // bit, 2)
        bit *= 2
    return peer


def spread_kernel(
    n, fk_ref, sk_ref, fv_ref, sv_ref, q_ref, sizes_ref, out_ref,
    stage, got_q, got_kv, att,
    load_sem, own_sem, send_sem, recv_sem, back_send, back_recv,
):
    rows, columns = q_ref.shape
    hd = columns // H
    me = lax.axis_index("seq")
    head = lax.rem(me, H)
    base = me - head
    keys = n * rows
    queries = H * rows

    loads = []
    for i, ref in enumerate((fk_ref, sk_ref, fv_ref, sv_ref, q_ref)):
        c = pltpu.make_async_copy(ref, stage.at[i], load_sem.at[i])
        c.start()
        loads.append(c)

    barrier = pltpu.get_barrier_semaphore()
    each(n, lambda k: pl.semaphore_signal(
        barrier, inc=1, device_id={"seq": flipped(me, k, n)}, device_id_type=MESH))
    pl.semaphore_wait(barrier, n - 1)

    def cols(h):
        return pl.ds(pl.multiple_of(h * hd, hd), hd)

    def at(p):
        return pl.ds(pl.multiple_of(p * rows, rows), rows)

    def views(phase, peer_head, source):
        if phase == 0:
            return stage.at[0:4, :, cols(peer_head)], got_kv.at[:, at(source), :]
        return stage.at[4, :, cols(peer_head)], got_q.at[at(lax.rem(source, H)), :]

    def remote(phase, peer, source, slot):
        src, dst = views(phase, lax.rem(peer, H), source)
        return pltpu.make_async_remote_copy(
            src_ref=src, dst_ref=dst,
            send_sem=send_sem.at[phase, slot], recv_sem=recv_sem.at[phase, slot],
            device_id={"seq": peer}, device_id_type=MESH)

    def own(phase):
        src, dst = views(phase, head, me)
        return pltpu.make_async_copy(src, dst, own_sem.at[phase])

    loads[4].wait()
    each(H, lambda k: remote(1, base + flipped(head, k, H), me, k).start())
    own(1).start()
    for i in range(4):
        loads[i].wait()
    each(n, lambda k: remote(0, flipped(me, k, n), me, k).start())
    own(0).start()

    ends, total = [], 0
    for p in range(sizes_ref.shape[0] - 1):
        total = total + sizes_ref[p]
        ends.append(total)

    block = 4 * rows
    scale = hd ** (-0.5)
    contract = (((1,), (1,)), ((), ()))

    def attend(b):
        at_b = pl.ds(pl.multiple_of(b * block, block), block)
        token = base * rows + b * block + lax.broadcasted_iota(jnp.int32, (block, 1), 0)
        limit = jnp.full((block, 1), keys, jnp.int32)
        for e in reversed(ends):
            limit = jnp.where(token < e, e, limit)
        fresh = lax.broadcasted_iota(jnp.int32, (block, keys), 1) < limit
        qb = got_q[at_b, :]
        sf = lax.dot_general(qb, got_kv[0], contract, preferred_element_type=jnp.float32)
        ss = lax.dot_general(qb, got_kv[1], contract, preferred_element_type=jnp.float32)
        s = jnp.where(fresh, sf, ss)
        w = jnp.exp((s - jnp.max(s, axis=1, keepdims=True)) * scale)
        den = jnp.sum(w, axis=1, keepdims=True)
        zero = jnp.zeros_like(w)
        wf = jnp.where(fresh, w, zero).astype(jnp.bfloat16)
        ws = jnp.where(fresh, zero, w).astype(jnp.bfloat16)
        num = jnp.dot(wf, got_kv[2], preferred_element_type=jnp.float32)
        num = num + jnp.dot(ws, got_kv[3], preferred_element_type=jnp.float32)
        att[at_b, :] = (num / den).astype(jnp.bfloat16)

    def back(slot):
        j = flipped(head, slot, H)
        return pltpu.make_async_remote_copy(
            src_ref=att.at[at(j), :], dst_ref=out_ref.at[:, cols(head)],
            send_sem=back_send.at[slot], recv_sem=back_recv.at[slot],
            device_id={"seq": base + j}, device_id_type=MESH)

    back_own = pltpu.make_async_copy(att.at[at(head), :], out_ref.at[:, cols(head)], own_sem.at[2])

    each(n, lambda k: remote(0, me, me, k).wait_recv())
    own(0).wait()
    for k in (2, 3, 1, 0):
        for slot in range(4 * k, 4 * k + 4):
            if slot:
                remote(1, me, me, slot).wait_recv()
            else:
                own(1).wait()
        attend(flipped(head // 4, k, H // 4))
        for slot in range(4 * k, 4 * k + 4):
            if slot:
                back(slot).start()
            else:
                back_own.start()

    each(n, lambda k: remote(0, me, me, k).wait_send())
    each(H, lambda k: remote(1, me, me, k).wait_send())
    for slot in range(1, H):
        back(slot).wait()
    back_own.wait()


def spread_shards(queries, fresh_keys, fresh_values, stale_keys, stale_values, patch_sizes):
    rows, columns = queries.shape
    n = lax.axis_size("seq")
    hd = columns // H
    keys, count = n * rows, H * rows
    dma = pltpu.SemaphoreType.DMA
    any_spec = pl.BlockSpec(memory_space=pl.ANY)
    return pl.pallas_call(
        functools.partial(spread_kernel, n),
        out_shape=pltpu.VMEM((rows, columns), queries.dtype),
        in_specs=[any_spec] * 5 + [pl.BlockSpec(memory_space=pltpu.SMEM)],
        out_specs=pl.BlockSpec(memory_space=pltpu.VMEM),
        scratch_shapes=[
            pltpu.VMEM((5, rows, columns), queries.dtype),
            pltpu.VMEM((count, hd), queries.dtype),
            pltpu.VMEM((4, keys, hd), queries.dtype),
            pltpu.VMEM((count, hd), queries.dtype),
            dma((5,)), dma((3,)), dma((2, n)), dma((2, n)), dma((H,)), dma((H,)),
        ],
        compiler_params=pltpu.CompilerParams(collective_id=0, has_side_effects=True),
    )(fresh_keys, stale_keys, fresh_values, stale_values, queries, patch_sizes)


def wave(i):
    return i // 4 + lax.rem(i // 2, 2)


def kernel(
    n, fk_ref, sk_ref, fv_ref, sv_ref, q_ref, sizes_hbm, out_ref,
    stage, got_q, got_kv, att, sizes_ref,
    load_sem, own_sem, send_sem, recv_sem, back_send, back_recv, ready,
):
    rows, columns = q_ref.shape
    hd = columns // H
    me = lax.axis_index("seq")
    keys = n * rows

    loads = []
    for i, ref in enumerate((fk_ref, sk_ref, fv_ref, sv_ref, q_ref)):
        c = pltpu.make_async_copy(ref, stage.at[i], load_sem.at[i])
        c.start()
        loads.append(c)
    load_sizes = pltpu.make_async_copy(sizes_hbm, sizes_ref, load_sem.at[5])
    load_sizes.start()

    def signal(sem, peer):
        pl.semaphore_signal(sem, inc=1, device_id={"seq": peer}, device_id_type=MESH)

    def others(body, far=False):
        for d in (range(n - 1, 0, -1) if far else range(1, n)):
            for peer, there in ((me + d, me + d < n), (me - d, me >= d)):
                body(jnp.where(there, peer, me), there)

    mine = wave(me)
    barrier = pltpu.get_barrier_semaphore()

    def greet(peer, there):
        pl.when(there & (wave(peer) >= mine))(lambda: signal(barrier, peer))

    others(greet)
    pl.semaphore_wait(barrier, jnp.minimum(4 * mine + 2, n) - 1)

    def answer(peer, there):
        pl.when(there & (wave(peer) < mine))(lambda: signal(ready.at[me], peer))

    others(answer)

    def cols(h):
        return pl.ds(pl.multiple_of(h * hd, hd), hd)

    def at(p):
        return pl.ds(pl.multiple_of(p * rows, rows), rows)

    def views(phase, peer, source):
        if phase == 0:
            return stage.at[0:4, :, cols(peer)], got_kv.at[:, at(source), :]
        return stage.at[4, :, cols(peer)], got_q.at[at(source), :]

    def remote(phase, peer, source, slot):
        src, dst = views(phase, peer, source)
        return pltpu.make_async_remote_copy(
            src_ref=src, dst_ref=dst,
            send_sem=send_sem.at[phase, peer], recv_sem=recv_sem.at[phase, slot],
            device_id={"seq": peer}, device_id_type=MESH)

    def own(phase):
        src, dst = views(phase, me, me)
        return pltpu.make_async_copy(src, dst, own_sem.at[phase])

    for i in range(4):
        loads[i].wait()

    def send_met(peer, there):
        pl.when(there & (wave(peer) <= mine))(lambda: remote(0, peer, me, me).start())

    def send_later(peer, there):
        def go():
            pl.semaphore_wait(ready.at[peer], 1)
            remote(0, peer, me, me).start()

        pl.when(there & (wave(peer) > mine))(go)

    def send_q(peer, there):
        pl.when(there)(lambda: remote(1, peer, me, me).start())

    others(send_met, far=True)
    others(send_later)
    loads[4].wait()
    others(send_q)
    own(0).start()
    own(1).start()
    load_sizes.wait()

    ends, total = [], 0
    for p in range(sizes_ref.shape[0] - 1):
        total = total + sizes_ref[p]
        ends.append(total)

    block = 4 * rows
    scale = hd ** (-0.5)
    contract = (((1,), (1,)), ((), ()))

    def attend(b):
        at_b = pl.ds(b * block, block)
        token = b * block + lax.broadcasted_iota(jnp.int32, (block, 1), 0)
        limit = jnp.full((block, 1), keys, jnp.int32)
        for e in reversed(ends):
            limit = jnp.where(token < e, e, limit)
        fresh = lax.broadcasted_iota(jnp.int32, (block, keys), 1) < limit
        qb = got_q[at_b, :]
        sf = lax.dot_general(qb, got_kv[0], contract, preferred_element_type=jnp.float32)
        ss = lax.dot_general(qb, got_kv[1], contract, preferred_element_type=jnp.float32)
        s = jnp.where(fresh, sf, ss)
        w = jnp.exp((s - jnp.max(s, axis=1, keepdims=True)) * scale)
        den = jnp.sum(w, axis=1, keepdims=True)
        zero = jnp.zeros_like(w)
        wf = jnp.where(fresh, w, zero).astype(jnp.bfloat16)
        ws = jnp.where(fresh, zero, w).astype(jnp.bfloat16)
        num = jnp.dot(wf, got_kv[2], preferred_element_type=jnp.float32)
        num = num + jnp.dot(ws, got_kv[3], preferred_element_type=jnp.float32)
        att[at_b, :] = (num / den).astype(jnp.bfloat16)

    def back(peer, source):
        return pltpu.make_async_remote_copy(
            src_ref=att.at[at(peer), :], dst_ref=out_ref.at[:, cols(source)],
            send_sem=back_send.at[peer], recv_sem=back_recv.at[source],
            device_id={"seq": peer}, device_id_type=MESH)

    back_own = pltpu.make_async_copy(att.at[at(me), :], out_ref.at[:, cols(me)], own_sem.at[2])

    def by_peer(sources, body, mine):
        for j in sources:
            pl.when(me != j)(functools.partial(body, j))
            pl.when(me == j)(mine)

    by_peer(range(n), lambda j: remote(0, me, j, j).wait_recv(), own(0).wait)
    for b in range(n // 4):
        group = range(4 * b, 4 * b + 4)
        by_peer(group, lambda j: remote(1, me, j, j).wait_recv(), own(1).wait)
        attend(b)
        by_peer(group, lambda j: back(j, me).start(), back_own.start)

    def drain(peer, there):
        def go():
            remote(0, peer, me, me).wait_send()
            remote(1, peer, me, me).wait_send()
            back(peer, me).wait_send()
            back(me, peer).wait_recv()

        pl.when(there)(go)

    others(drain)
    back_own.wait()


def shards(queries, fresh_keys, fresh_values, stale_keys, stale_values, patch_sizes):
    rows, columns = queries.shape
    n = lax.axis_size("seq")
    hd = columns // H
    keys = n * rows
    dma = pltpu.SemaphoreType.DMA
    return pl.pallas_call(
        functools.partial(kernel, n),
        out_shape=pltpu.VMEM((rows, columns), queries.dtype),
        in_specs=[pl.BlockSpec(memory_space=pl.ANY)] * 6,
        out_specs=pl.BlockSpec(memory_space=pltpu.VMEM),
        scratch_shapes=[
            pltpu.VMEM((5, rows, columns), queries.dtype),
            pltpu.VMEM((keys, hd), queries.dtype),
            pltpu.VMEM((4, keys, hd), queries.dtype),
            pltpu.VMEM((keys, hd), queries.dtype),
            pltpu.SMEM(patch_sizes.shape, patch_sizes.dtype),
            dma((6,)), dma((3,)), dma((2, n)), dma((2, n)), dma((n,)), dma((n,)),
            pltpu.SemaphoreType.REGULAR((n,)),
        ],
        compiler_params=pltpu.CompilerParams(collective_id=0, has_side_effects=True),
    )(fresh_keys, stale_keys, fresh_values, stale_values, queries, patch_sizes)


def solution(mesh):
    spec = P(("groups", "seq"), None)
    body = shards if mesh.shape["seq"] == H else spread_shards
    return jax.shard_map(
        body, mesh=mesh, in_specs=(spec,) * 5 + (P("groups"),), out_specs=spec, check_vma=False)
```

```python
import functools

import jax
import jax.numpy as jnp
from jax import lax
from jax.experimental import pallas as pl
from jax.experimental.pallas import tpu as pltpu
from jax.sharding import PartitionSpec as P

H = 16
MESH = pl.DeviceIdType.MESH


def each(count, body):
    if count <= 32:
        for k in range(1, count):
            body(k)
    else:
        lax.fori_loop(1, count, lambda k, c: (body(k), c)[1], 0)


def flipped(me, k, count):
    if count & (count - 1):
        return lax.rem(me + k, count)
    peer, bit = 0, 1
    while bit < count:
        peer = peer + bit * lax.rem(me // bit + k // bit, 2)
        bit *= 2
    return peer


def spread_kernel(
    n, fk_ref, sk_ref, fv_ref, sv_ref, q_ref, sizes_ref, out_ref,
    stage, got_q, got_kv, att,
    load_sem, own_sem, send_sem, recv_sem, back_send, back_recv,
):
    rows, columns = q_ref.shape
    hd = columns // H
    me = lax.axis_index("seq")
    head = lax.rem(me, H)
    base = me - head
    keys = n * rows
    queries = H * rows

    loads = []
    for i, ref in enumerate((fk_ref, sk_ref, fv_ref, sv_ref, q_ref)):
        c = pltpu.make_async_copy(ref, stage.at[i], load_sem.at[i])
        c.start()
        loads.append(c)

    barrier = pltpu.get_barrier_semaphore()
    each(n, lambda k: pl.semaphore_signal(
        barrier, inc=1, device_id={"seq": flipped(me, k, n)}, device_id_type=MESH))
    pl.semaphore_wait(barrier, n - 1)

    def cols(h):
        return pl.ds(pl.multiple_of(h * hd, hd), hd)

    def at(p):
        return pl.ds(pl.multiple_of(p * rows, rows), rows)

    def views(phase, peer_head, source):
        if phase == 0:
            return stage.at[0:4, :, cols(peer_head)], got_kv.at[:, at(source), :]
        return stage.at[4, :, cols(peer_head)], got_q.at[at(lax.rem(source, H)), :]

    def remote(phase, peer, source, slot):
        src, dst = views(phase, lax.rem(peer, H), source)
        return pltpu.make_async_remote_copy(
            src_ref=src, dst_ref=dst,
            send_sem=send_sem.at[phase, slot], recv_sem=recv_sem.at[phase, slot],
            device_id={"seq": peer}, device_id_type=MESH)

    def own(phase):
        src, dst = views(phase, head, me)
        return pltpu.make_async_copy(src, dst, own_sem.at[phase])

    loads[4].wait()
    each(H, lambda k: remote(1, base + flipped(head, k, H), me, k).start())
    own(1).start()
    for i in range(4):
        loads[i].wait()
    each(n, lambda k: remote(0, flipped(me, k, n), me, k).start())
    own(0).start()

    ends, total = [], 0
    for p in range(sizes_ref.shape[0] - 1):
        total = total + sizes_ref[p]
        ends.append(total)

    block = 4 * rows
    scale = hd ** (-0.5)
    contract = (((1,), (1,)), ((), ()))

    def attend(b):
        at_b = pl.ds(pl.multiple_of(b * block, block), block)
        token = base * rows + b * block + lax.broadcasted_iota(jnp.int32, (block, 1), 0)
        limit = jnp.full((block, 1), keys, jnp.int32)
        for e in reversed(ends):
            limit = jnp.where(token < e, e, limit)
        fresh = lax.broadcasted_iota(jnp.int32, (block, keys), 1) < limit
        qb = got_q[at_b, :]
        sf = lax.dot_general(qb, got_kv[0], contract, preferred_element_type=jnp.float32)
        ss = lax.dot_general(qb, got_kv[1], contract, preferred_element_type=jnp.float32)
        s = jnp.where(fresh, sf, ss)
        w = jnp.exp((s - jnp.max(s, axis=1, keepdims=True)) * scale)
        den = jnp.sum(w, axis=1, keepdims=True)
        zero = jnp.zeros_like(w)
        wf = jnp.where(fresh, w, zero).astype(jnp.bfloat16)
        ws = jnp.where(fresh, zero, w).astype(jnp.bfloat16)
        num = jnp.dot(wf, got_kv[2], preferred_element_type=jnp.float32)
        num = num + jnp.dot(ws, got_kv[3], preferred_element_type=jnp.float32)
        att[at_b, :] = (num / den).astype(jnp.bfloat16)

    def back(slot):
        j = flipped(head, slot, H)
        return pltpu.make_async_remote_copy(
            src_ref=att.at[at(j), :], dst_ref=out_ref.at[:, cols(head)],
            send_sem=back_send.at[slot], recv_sem=back_recv.at[slot],
            device_id={"seq": base + j}, device_id_type=MESH)

    back_own = pltpu.make_async_copy(att.at[at(head), :], out_ref.at[:, cols(head)], own_sem.at[2])

    each(n, lambda k: remote(0, me, me, k).wait_recv())
    own(0).wait()
    for k in (2, 3, 1, 0):
        for slot in range(4 * k, 4 * k + 4):
            if slot:
                remote(1, me, me, slot).wait_recv()
            else:
                own(1).wait()
        attend(flipped(head // 4, k, H // 4))
        for slot in range(4 * k, 4 * k + 4):
            if slot:
                back(slot).start()
            else:
                back_own.start()

    each(n, lambda k: remote(0, me, me, k).wait_send())
    each(H, lambda k: remote(1, me, me, k).wait_send())
    for slot in range(1, H):
        back(slot).wait()
    back_own.wait()


def spread_shards(queries, fresh_keys, fresh_values, stale_keys, stale_values, patch_sizes):
    rows, columns = queries.shape
    n = lax.axis_size("seq")
    hd = columns // H
    keys, count = n * rows, H * rows
    dma = pltpu.SemaphoreType.DMA
    any_spec = pl.BlockSpec(memory_space=pl.ANY)
    return pl.pallas_call(
        functools.partial(spread_kernel, n),
        out_shape=pltpu.VMEM((rows, columns), queries.dtype),
        in_specs=[any_spec] * 5 + [pl.BlockSpec(memory_space=pltpu.SMEM)],
        out_specs=pl.BlockSpec(memory_space=pltpu.VMEM),
        scratch_shapes=[
            pltpu.VMEM((5, rows, columns), queries.dtype),
            pltpu.VMEM((count, hd), queries.dtype),
            pltpu.VMEM((4, keys, hd), queries.dtype),
            pltpu.VMEM((count, hd), queries.dtype),
            dma((5,)), dma((3,)), dma((2, n)), dma((2, n)), dma((H,)), dma((H,)),
        ],
        compiler_params=pltpu.CompilerParams(collective_id=0, has_side_effects=True),
    )(fresh_keys, stale_keys, fresh_values, stale_values, queries, patch_sizes)


def kernel(
    n, fk_ref, sk_ref, fv_ref, sv_ref, q_ref, sizes_hbm, out_ref,
    stage, got_q, got_kv, turned, att, lse_out, part, lse_in, mix, sizes_ref,
    load_sem, kv_recv, q_recv, o_recv, l_recv, kv_send, q_send, o_send, l_send, ready,
):
    rows, columns = q_ref.shape
    hd = columns // H
    me = lax.axis_index("seq")
    half = n // 2
    held = H // half
    keys = half * rows
    lanes = lse_in.shape[2]
    per = lanes // rows
    chips = n // 2
    side = me // half

    for i, ref in enumerate((fk_ref, sk_ref, fv_ref, sv_ref, q_ref)):
        pltpu.make_async_copy(ref, stage.at[i], load_sem.at[0]).start()
    load_sizes = pltpu.make_async_copy(sizes_hbm, sizes_ref, load_sem.at[1])
    load_sizes.start()

    def wave(i):
        return i // 4 + lax.rem(i // 2, 2)

    def signal(sem, peer):
        pl.semaphore_signal(sem, inc=1, device_id={"seq": peer}, device_id_type=MESH)

    mine, chip = wave(me), me // 2
    upper = lax.rem(chip, 2) == 1
    buddy = 2 * chip + 1 - lax.rem(me, 2)
    barrier = pltpu.get_barrier_semaphore()
    signal(barrier, buddy)
    for d in range(1, n):
        peer = me + d
        pl.when((peer < n) & (wave(peer) > mine))(functools.partial(signal, barrier, jnp.where(peer < n, peer, me)))
    pl.semaphore_wait(barrier, jnp.maximum(4 * mine - 2, 0) + 1)
    for d in range(1, n):
        peer = me - d
        pl.when((peer >= 0) & (wave(peer) < mine))(functools.partial(signal, ready.at[chip], jnp.maximum(peer, 0)))

    def cols(h, count=1):
        return pl.ds(pl.multiple_of(h * hd, hd), count * hd)

    def at(p, count=1):
        return pl.ds(pl.multiple_of(p * rows, rows), count * rows)

    def to(peer, src, dst, send, recv):
        return pltpu.make_async_remote_copy(
            src_ref=src, dst_ref=dst, send_sem=send, recv_sem=recv,
            device_id={"seq": peer}, device_id_type=MESH)

    def kv_views(a, peer):
        return (stage.at[0:4, :, cols(lax.rem(peer, half) * held + a)],
                got_kv.at[a, :, at(lax.rem(me, half)), :])

    def q_views(peer):
        return stage.at[4, :, cols(lax.rem(peer, half) * held, held)], got_q.at[at(me), :]

    def o_views(a, peer):
        return (att.at[at(peer), a * hd:(a + 1) * hd],
                part.at[side, :, cols(lax.rem(me, half) * held + a)])

    def l_views(peer):
        return lse_out.at[peer // per], lse_in.at[me]

    def send_kv(a, peer):
        to(peer, *kv_views(a, peer), kv_send.at[0], kv_recv.at[a]).start()

    def send_q(peer):
        to(peer, *q_views(peer), q_send.at[0], q_recv.at[side]).start()

    def send_o(a, peer):
        to(peer, *o_views(a, peer), o_send.at[0], o_recv.at[0]).start()

    def send_l(peer):
        to(peer, *l_views(peer), l_send.at[0], l_recv.at[0]).start()

    def arrived(sem, ref):
        to(me, ref, ref, sem, sem).wait_recv()

    def left(sem, ref):
        to(me, ref, ref, sem, sem).wait_send()

    def keep(src, dst):
        dst[...] = src[...]

    def cores(target, cond, body):
        @pl.when(cond)
        def _():
            for core in range(2):
                body(2 * jnp.clip(target, 0, chips - 1) + core)

    def near(target):
        return target // (chips // 2) == side

    def tied(target):
        return (upper & (target == chip + 1)) | (jnp.logical_not(upper) & (target == chip - 1))

    def met(body, same):
        for e in range(1, chips):
            t = chip - e
            cores(t, (t >= 0) & jnp.logical_not(tied(t)) & (near(t) == same), body)

    def heard(body):
        for e in range(1, chips):
            t = chip + e
            cores(t, (t < chips) & jnp.logical_not(tied(t)) & near(t), body)
        for t in (chip - 1, chip + 1):
            cores(t, (t >= 0) & (t < chips) & tied(t) & near(t), body)

    arrived(load_sem.at[0], stage)
    def met_q():
        send_q(buddy)
        met(send_q, True)

    for a in range(held):
        send_kv(a, buddy)
        met(functools.partial(send_kv, a), True)
        if a == 0:
            pl.when(side == 0)(met_q)
    met(send_q, False)

    def first(target, cond):
        cores(target, cond & near(target), functools.partial(send_kv, 0))
        cores(target, cond & ((side == 0) | jnp.logical_not(near(target))), send_q)

    for e in range(1, chips):
        t = chip + e
        there = (t < chips) & jnp.logical_not(tied(t))

        @pl.when(there)
        def _():
            pl.semaphore_wait(ready.at[t], 2)

        first(t, there)
        if e == 1:
            t = chip - 1
            first(t, (t >= 0) & tied(t))
        if e == 2:
            t = chip + 1
            first(t, (t < chips) & tied(t))
    for a in range(1, held):
        heard(functools.partial(send_kv, a))

    def late_q():
        met_q()
        heard(send_q)

    pl.when(side == 1)(late_q)
    for a in range(held):
        keep(*kv_views(a, me))
    keep(*q_views(me))
    load_sizes.wait()

    ends, total = [], 0
    for p in range(sizes_ref.shape[0] - 1):
        total = total + sizes_ref[p]
        ends.append(total)

    scale = hd ** (-0.5) * 1.4426950408889634
    contract = (((1,), (1,)), ((), ()))

    def turn(a):
        turned[a, :, 0:keys] = got_kv[a, 2].T
        turned[a, :, keys:2 * keys] = got_kv[a, 3].T

    def attend(a, s):
        token = s * keys + lax.broadcasted_iota(jnp.int32, (1, keys), 1)
        limit = jnp.full((1, keys), 2 * keys, jnp.int32)
        for e in reversed(ends):
            limit = jnp.where(token < e, e, limit)
        fresh = lax.broadcasted_iota(jnp.int32, (keys, keys), 0) < limit - side * keys
        both = got_kv[a, 0:2].reshape(2 * keys, hd)
        qb = got_q[s * keys:(s + 1) * keys, a * hd:(a + 1) * hd]
        x = lax.dot_general(both, qb, contract, preferred_element_type=jnp.float32)
        x = jnp.where(fresh, x[:keys], x[keys:])
        top = jnp.max(x, axis=0, keepdims=True)
        w = jnp.exp2((x - top) * scale)
        den = jnp.sum(w, axis=0, keepdims=True)
        zero = jnp.zeros_like(w)
        wf = jnp.where(fresh, w, zero).astype(jnp.bfloat16)
        ws = jnp.where(fresh, zero, w).astype(jnp.bfloat16)
        num = jnp.dot(turned[a], jnp.concatenate([wf, ws], axis=0), preferred_element_type=jnp.float32)
        att[s * keys:(s + 1) * keys, a * hd:(a + 1) * hd] = (num * (1.0 / den)).T.astype(jnp.bfloat16)
        lse = top * scale + jnp.log2(den)
        for b in range(keys // lanes):
            lse_out[s * (keys // lanes) + b, a:a + 1, :] = lse[:, b * lanes:(b + 1) * lanes]

    def give(s, body, own):
        for j in range(s * half, (s + 1) * half):
            pl.when(me != j)(functools.partial(body, j))
        pl.when(side == s)(own)

    def give_o(a, s):
        give(s, functools.partial(send_o, a), lambda: keep(*o_views(a, me)))

    def give_l(s):
        give(s, send_l, lambda: keep(*l_views(me)))

    def wait_q(s):
        pl.when(side == s)(lambda: arrived(q_recv.at[s], got_q.at[0:(half - 1) * rows, :]))
        pl.when(side != s)(lambda: arrived(q_recv.at[s], got_q.at[0:half * rows, :]))

    for a in range(held):
        arrived(kv_recv.at[a], got_kv.at[a, :, 0:(half - 1) * rows, :])
        turn(a)
        if a == 0:
            wait_q(0)
        attend(a, 0)
        if a == held - 1:
            give_l(0)
        give_o(a, 0)
    wait_q(1)
    for a in range(held):
        attend(a, 1)
        if a == held - 1:
            give_l(1)
        give_o(a, 1)

    most = (n - 1) * rows
    arrived(o_recv.at[0], att.at[0:most, :])
    arrived(l_recv.at[0], lse_in.at[0:n - 1])
    low = lse_in[0:half].reshape(H, lanes)
    high = lse_in[half:n].reshape(H, lanes)
    top = jnp.maximum(low, high)
    low, high = jnp.exp2(low - top), jnp.exp2(high - top)
    total = low + high
    fill = jnp.zeros((lanes - 2 * H, lanes), jnp.float32)
    mix[...] = jnp.concatenate([low / total, high / total, fill], axis=0).T
    share = mix[at(lax.rem(me, per)), :]
    for h in range(H):
        c = slice(h * hd, (h + 1) * hd)
        out = share[:, h:h + 1] * part[0, :, c].astype(jnp.float32)
        out = out + share[:, H + h:H + h + 1] * part[1, :, c].astype(jnp.float32)
        out_ref[:, c] = out.astype(out_ref.dtype)

    left(kv_send.at[0], got_kv.at[:, :, 0:(half - 1) * rows, :])
    left(q_send.at[0], got_q.at[0:most, :])
    left(o_send.at[0], att.at[0:most, :])
    left(l_send.at[0], lse_in.at[0:n - 1])


def shards(queries, fresh_keys, fresh_values, stale_keys, stale_values, patch_sizes):
    rows, columns = queries.shape
    n = lax.axis_size("seq")
    hd = columns // H
    half = n // 2
    held = H // half
    keys, lanes = half * rows, 128
    dma = pltpu.SemaphoreType.DMA
    kind = queries.dtype
    return pl.pallas_call(
        functools.partial(kernel, n),
        out_shape=pltpu.VMEM((rows, columns), kind),
        in_specs=[pl.BlockSpec(memory_space=pl.ANY)] * 6,
        out_specs=pl.BlockSpec(memory_space=pltpu.VMEM),
        scratch_shapes=[
            pltpu.VMEM((5, rows, columns), kind),
            pltpu.VMEM((n * rows, held * hd), kind),
            pltpu.VMEM((held, 4, keys, hd), kind),
            pltpu.VMEM((held, hd, 2 * keys), kind),
            pltpu.VMEM((n * rows, held * hd), kind),
            pltpu.VMEM((n * rows // lanes, held, lanes), jnp.float32),
            pltpu.VMEM((2, rows, columns), kind),
            pltpu.VMEM((n, held, lanes), jnp.float32),
            pltpu.VMEM((lanes, lanes), jnp.float32),
            pltpu.SMEM(patch_sizes.shape, patch_sizes.dtype),
            dma((2,)), dma((held,)), dma((2,)), dma((1,)), dma((1,)),
            dma((1,)), dma((1,)), dma((1,)), dma((1,)),
            pltpu.SemaphoreType.REGULAR((n // 2,)),
        ],
        compiler_params=pltpu.CompilerParams(collective_id=0, has_side_effects=True),
    )(fresh_keys, stale_keys, fresh_values, stale_values, queries, patch_sizes)


def solution(mesh):
    spec = P(("groups", "seq"), None)
    body = shards if mesh.shape["seq"] == H else spread_shards
    return jax.shard_map(
        body, mesh=mesh, in_specs=(spec,) * 5 + (P("groups"),), out_specs=spec, check_vma=False)
```

```python
import functools

import jax
import jax.numpy as jnp
from jax import lax
from jax.experimental import pallas as pl
from jax.experimental.pallas import tpu as pltpu
from jax.sharding import PartitionSpec as P

H = 16
MESH = pl.DeviceIdType.MESH


def each(count, body):
    if count <= 32:
        for k in range(1, count):
            body(k)
    else:
        lax.fori_loop(1, count, lambda k, c: (body(k), c)[1], 0)


def flipped(me, k, count):
    if count & (count - 1):
        return lax.rem(me + k, count)
    peer, bit = 0, 1
    while bit < count:
        peer = peer + bit * lax.rem(me // bit + k // bit, 2)
        bit *= 2
    return peer


def spread_kernel(
    n, fk_ref, sk_ref, fv_ref, sv_ref, q_ref, sizes_ref, out_ref,
    stage, got_q, got_kv, att,
    load_sem, own_sem, send_sem, recv_sem, back_send, back_recv,
):
    rows, columns = q_ref.shape
    hd = columns // H
    me = lax.axis_index("seq")
    head = lax.rem(me, H)
    base = me - head
    keys = n * rows
    queries = H * rows

    loads = []
    for i, ref in enumerate((fk_ref, sk_ref, fv_ref, sv_ref, q_ref)):
        c = pltpu.make_async_copy(ref, stage.at[i], load_sem.at[i])
        c.start()
        loads.append(c)

    barrier = pltpu.get_barrier_semaphore()
    each(n, lambda k: pl.semaphore_signal(
        barrier, inc=1, device_id={"seq": flipped(me, k, n)}, device_id_type=MESH))
    pl.semaphore_wait(barrier, n - 1)

    def cols(h):
        return pl.ds(pl.multiple_of(h * hd, hd), hd)

    def at(p):
        return pl.ds(pl.multiple_of(p * rows, rows), rows)

    def views(phase, peer_head, source):
        if phase == 0:
            return stage.at[0:4, :, cols(peer_head)], got_kv.at[:, at(source), :]
        return stage.at[4, :, cols(peer_head)], got_q.at[at(lax.rem(source, H)), :]

    def remote(phase, peer, source, slot):
        src, dst = views(phase, lax.rem(peer, H), source)
        return pltpu.make_async_remote_copy(
            src_ref=src, dst_ref=dst,
            send_sem=send_sem.at[phase, slot], recv_sem=recv_sem.at[phase, slot],
            device_id={"seq": peer}, device_id_type=MESH)

    def own(phase):
        src, dst = views(phase, head, me)
        return pltpu.make_async_copy(src, dst, own_sem.at[phase])

    loads[4].wait()
    each(H, lambda k: remote(1, base + flipped(head, k, H), me, k).start())
    own(1).start()
    for i in range(4):
        loads[i].wait()
    each(n, lambda k: remote(0, flipped(me, k, n), me, k).start())
    own(0).start()

    ends, total = [], 0
    for p in range(sizes_ref.shape[0] - 1):
        total = total + sizes_ref[p]
        ends.append(total)

    block = 4 * rows
    scale = hd ** (-0.5)
    contract = (((1,), (1,)), ((), ()))

    def attend(b):
        at_b = pl.ds(pl.multiple_of(b * block, block), block)
        token = base * rows + b * block + lax.broadcasted_iota(jnp.int32, (block, 1), 0)
        limit = jnp.full((block, 1), keys, jnp.int32)
        for e in reversed(ends):
            limit = jnp.where(token < e, e, limit)
        fresh = lax.broadcasted_iota(jnp.int32, (block, keys), 1) < limit
        qb = got_q[at_b, :]
        sf = lax.dot_general(qb, got_kv[0], contract, preferred_element_type=jnp.float32)
        ss = lax.dot_general(qb, got_kv[1], contract, preferred_element_type=jnp.float32)
        s = jnp.where(fresh, sf, ss)
        w = jnp.exp((s - jnp.max(s, axis=1, keepdims=True)) * scale)
        den = jnp.sum(w, axis=1, keepdims=True)
        zero = jnp.zeros_like(w)
        wf = jnp.where(fresh, w, zero).astype(jnp.bfloat16)
        ws = jnp.where(fresh, zero, w).astype(jnp.bfloat16)
        num = jnp.dot(wf, got_kv[2], preferred_element_type=jnp.float32)
        num = num + jnp.dot(ws, got_kv[3], preferred_element_type=jnp.float32)
        att[at_b, :] = (num / den).astype(jnp.bfloat16)

    def back(slot):
        j = flipped(head, slot, H)
        return pltpu.make_async_remote_copy(
            src_ref=att.at[at(j), :], dst_ref=out_ref.at[:, cols(head)],
            send_sem=back_send.at[slot], recv_sem=back_recv.at[slot],
            device_id={"seq": base + j}, device_id_type=MESH)

    back_own = pltpu.make_async_copy(att.at[at(head), :], out_ref.at[:, cols(head)], own_sem.at[2])

    each(n, lambda k: remote(0, me, me, k).wait_recv())
    own(0).wait()
    for k in (2, 3, 1, 0):
        for slot in range(4 * k, 4 * k + 4):
            if slot:
                remote(1, me, me, slot).wait_recv()
            else:
                own(1).wait()
        attend(flipped(head // 4, k, H // 4))
        for slot in range(4 * k, 4 * k + 4):
            if slot:
                back(slot).start()
            else:
                back_own.start()

    each(n, lambda k: remote(0, me, me, k).wait_send())
    each(H, lambda k: remote(1, me, me, k).wait_send())
    for slot in range(1, H):
        back(slot).wait()
    back_own.wait()


def spread_shards(queries, fresh_keys, fresh_values, stale_keys, stale_values, patch_sizes):
    rows, columns = queries.shape
    n = lax.axis_size("seq")
    hd = columns // H
    keys, count = n * rows, H * rows
    dma = pltpu.SemaphoreType.DMA
    any_spec = pl.BlockSpec(memory_space=pl.ANY)
    return pl.pallas_call(
        functools.partial(spread_kernel, n),
        out_shape=pltpu.VMEM((rows, columns), queries.dtype),
        in_specs=[any_spec] * 5 + [pl.BlockSpec(memory_space=pltpu.SMEM)],
        out_specs=pl.BlockSpec(memory_space=pltpu.VMEM),
        scratch_shapes=[
            pltpu.VMEM((5, rows, columns), queries.dtype),
            pltpu.VMEM((count, hd), queries.dtype),
            pltpu.VMEM((4, keys, hd), queries.dtype),
            pltpu.VMEM((count, hd), queries.dtype),
            dma((5,)), dma((3,)), dma((2, n)), dma((2, n)), dma((H,)), dma((H,)),
        ],
        compiler_params=pltpu.CompilerParams(collective_id=0, has_side_effects=True),
    )(fresh_keys, stale_keys, fresh_values, stale_values, queries, patch_sizes)


def kernel(
    n, fk_ref, sk_ref, fv_ref, sv_ref, q_ref, sizes_hbm, out_ref,
    stage, got_q, got_kv, turned, att, lse_out, part, lse_in, mix, sizes_ref,
    load_sem, kv_recv, q_recv, o_recv, l_recv, kv_send, q_send, o_send, l_send, ready,
):
    rows, columns = q_ref.shape
    hd = columns // H
    me = lax.axis_index("seq")
    half = n // 2
    held = H // half
    keys = half * rows
    lanes = lse_in.shape[2]
    per = lanes // rows
    chips = n // 2
    side = me // half

    for i, ref in enumerate((fk_ref, sk_ref, fv_ref, sv_ref, q_ref)):
        pltpu.make_async_copy(ref, stage.at[i], load_sem.at[0]).start()
    load_sizes = pltpu.make_async_copy(sizes_hbm, sizes_ref, load_sem.at[1])
    load_sizes.start()

    def wave(i):
        return i // 4 + lax.rem(i // 2, 2)

    def signal(sem, peer):
        pl.semaphore_signal(sem, inc=1, device_id={"seq": peer}, device_id_type=MESH)

    mine, chip = wave(me), me // 2
    upper = lax.rem(chip, 2) == 1
    buddy = 2 * chip + 1 - lax.rem(me, 2)
    barrier = pltpu.get_barrier_semaphore()
    signal(barrier, buddy)
    for d in range(1, n):
        peer = me + d
        pl.when((peer < n) & (wave(peer) > mine))(functools.partial(signal, barrier, jnp.where(peer < n, peer, me)))
    pl.semaphore_wait(barrier, jnp.maximum(4 * mine - 2, 0) + 1)
    for d in range(1, n):
        peer = me - d
        pl.when((peer >= 0) & (wave(peer) < mine))(functools.partial(signal, ready.at[chip], jnp.maximum(peer, 0)))

    def cols(h, count=1):
        return pl.ds(pl.multiple_of(h * hd, hd), count * hd)

    def at(p, count=1):
        return pl.ds(pl.multiple_of(p * rows, rows), count * rows)

    def to(peer, src, dst, send, recv):
        return pltpu.make_async_remote_copy(
            src_ref=src, dst_ref=dst, send_sem=send, recv_sem=recv,
            device_id={"seq": peer}, device_id_type=MESH)

    def kv_views(a, peer):
        return (stage.at[0:4, :, cols(lax.rem(peer, half) * held + a)],
                got_kv.at[a, :, at(lax.rem(me, half)), :])

    def q_views(peer):
        return stage.at[4, :, cols(lax.rem(peer, half) * held, held)], got_q.at[at(me), :]

    def o_views(a, peer):
        return (att.at[at(peer), a * hd:(a + 1) * hd],
                part.at[side, :, cols(lax.rem(me, half) * held + a)])

    def l_views(peer):
        return lse_out.at[peer // per], lse_in.at[me]

    def send_kv(a, peer):
        to(peer, *kv_views(a, peer), kv_send.at[0], kv_recv.at[a]).start()

    def send_q(peer):
        to(peer, *q_views(peer), q_send.at[0], q_recv.at[me // per]).start()

    def send_o(a, peer):
        to(peer, *o_views(a, peer), o_send.at[0], o_recv.at[0]).start()

    def send_l(peer):
        to(peer, *l_views(peer), l_send.at[0], l_recv.at[0]).start()

    def arrived(sem, ref):
        to(me, ref, ref, sem, sem).wait_recv()

    def left(sem, ref):
        to(me, ref, ref, sem, sem).wait_send()

    def keep(src, dst):
        dst[...] = src[...]

    def cores(target, cond, body):
        @pl.when(cond)
        def _():
            for core in range(2):
                body(2 * jnp.clip(target, 0, chips - 1) + core)

    def near(target):
        return target // (chips // 2) == side

    def tied(target):
        return (upper & (target == chip + 1)) | (jnp.logical_not(upper) & (target == chip - 1))

    def met(body, same):
        for e in range(1, chips):
            t = chip - e
            cores(t, (t >= 0) & jnp.logical_not(tied(t)) & (near(t) == same), body)

    def heard(body):
        for e in range(1, chips):
            t = chip + e
            cores(t, (t < chips) & jnp.logical_not(tied(t)) & near(t), body)
        for t in (chip - 1, chip + 1):
            cores(t, (t >= 0) & (t < chips) & tied(t) & near(t), body)

    arrived(load_sem.at[0], stage)

    def met_q():
        send_q(buddy)
        met(send_q, True)

    def met_kv(a):
        send_kv(a, buddy)
        met(functools.partial(send_kv, a), True)

    def first(target, cond):
        cores(target, cond & near(target), functools.partial(send_kv, 0))
        cores(target, cond & ((side == 0) | jnp.logical_not(near(target))), send_q)

    met_kv(0)
    pl.when(side == 0)(met_q)
    for e in range(1, chips):
        t = chip + e
        there = (t < chips) & jnp.logical_not(tied(t))

        @pl.when(there)
        def _():
            pl.semaphore_wait(ready.at[t], 2)

        first(t, there)
        if e == 1:
            t = chip - 1
            first(t, (t >= 0) & tied(t))
        if e == 2:
            t = chip + 1
            first(t, (t < chips) & tied(t))
            met(send_q, False)
            for a in range(1, held):
                met_kv(a)
    for a in range(1, held):
        heard(functools.partial(send_kv, a))

    def late_q():
        met_q()
        heard(send_q)

    pl.when(side == 1)(late_q)
    for a in range(held):
        keep(*kv_views(a, me))
    keep(*q_views(me))
    load_sizes.wait()

    ends, total = [], 0
    for p in range(sizes_ref.shape[0] - 1):
        total = total + sizes_ref[p]
        ends.append(total)

    scale = hd ** (-0.5) * 1.4426950408889634
    contract = (((1,), (1,)), ((), ()))

    def turn(a):
        turned[a, :, 0:keys] = got_kv[a, 2].T
        turned[a, :, keys:2 * keys] = got_kv[a, 3].T

    def attend(a, start, count):
        at_q = slice(start, start + count)
        token = start + lax.broadcasted_iota(jnp.int32, (1, count), 1)
        limit = jnp.full((1, count), 2 * keys, jnp.int32)
        for e in reversed(ends):
            limit = jnp.where(token < e, e, limit)
        fresh = lax.broadcasted_iota(jnp.int32, (keys, count), 0) < limit - side * keys
        both = got_kv[a, 0:2].reshape(2 * keys, hd)
        qb = got_q[at_q, a * hd:(a + 1) * hd]
        x = lax.dot_general(both, qb, contract, preferred_element_type=jnp.float32)
        x = jnp.where(fresh, x[:keys], x[keys:])
        top = jnp.max(x, axis=0, keepdims=True)
        w = jnp.exp2((x - top) * scale)
        den = jnp.sum(w, axis=0, keepdims=True)
        zero = jnp.zeros_like(w)
        wf = jnp.where(fresh, w, zero).astype(jnp.bfloat16)
        ws = jnp.where(fresh, zero, w).astype(jnp.bfloat16)
        num = jnp.dot(turned[a], jnp.concatenate([wf, ws], axis=0), preferred_element_type=jnp.float32)
        att[at_q, a * hd:(a + 1) * hd] = (num * (1.0 / den)).T.astype(jnp.bfloat16)
        lse = top * scale + jnp.log2(den)
        for b in range(count // lanes):
            lse_out[start // lanes + b, a:a + 1, :] = lse[:, b * lanes:(b + 1) * lanes]

    def give(a, planes, last):
        for p in planes:
            for j in range(p * per, (p + 1) * per):
                @pl.when(me != j)
                def _(j=j):
                    if last:
                        send_l(j)
                    send_o(a, j)

    def own(a, last):
        if last:
            keep(*l_views(me))
        keep(*o_views(a, me))

    def work(a, planes, mine, last=False):
        attend(a, planes[0] * lanes, len(planes) * lanes)
        give(a, planes, last)
        if mine:
            own(a, last)

    def wait_kv(a):
        arrived(kv_recv.at[a], got_kv.at[a, :, 0:(half - 1) * rows, :])
        turn(a)

    def wait_q(planes, mine):
        for p in planes:
            if mine:
                pl.when(me // per == p)(lambda p=p: arrived(q_recv.at[p], got_q.at[0:(per - 1) * rows, :]))
                pl.when(me // per != p)(lambda p=p: arrived(q_recv.at[p], got_q.at[0:per * rows, :]))
            else:
                arrived(q_recv.at[p], got_q.at[0:per * rows, :])

    planes = n // per
    low_planes, high_planes = range(planes // 2), range(planes // 2, planes)
    end = held - 1

    @pl.when(side == 0)
    def _():
        wait_kv(0)
        wait_q(low_planes, True)
        work(0, low_planes, True)
        for p in high_planes[:-1]:
            wait_q([p], False)
            work(0, [p], False)
        for a in range(1, held):
            wait_kv(a)
            work(a, low_planes, True, a == end)
            for p in high_planes[:-1]:
                work(a, [p], False, a == end)
        wait_q(high_planes[-1:], False)
        for a in range(held):
            work(a, high_planes[-1:], False, a == end)

    @pl.when(side == 1)
    def _():
        for a in range(held):
            wait_kv(a)
            if a == 0:
                wait_q(low_planes, False)
            work(a, low_planes, False, a == end)
        wait_q(high_planes, True)
        for a in range(held):
            work(a, high_planes, True, a == end)

    most = (n - 1) * rows
    arrived(o_recv.at[0], att.at[0:most, :])
    arrived(l_recv.at[0], lse_in.at[0:n - 1])
    low = lse_in[0:half].reshape(H, lanes)
    high = lse_in[half:n].reshape(H, lanes)
    top = jnp.maximum(low, high)
    low, high = jnp.exp2(low - top), jnp.exp2(high - top)
    total = low + high
    fill = jnp.zeros((lanes - 2 * H, lanes), jnp.float32)
    mix[...] = jnp.concatenate([low / total, high / total, fill], axis=0).T
    share = mix[at(lax.rem(me, per)), :]
    for h in range(H):
        c = slice(h * hd, (h + 1) * hd)
        out = share[:, h:h + 1] * part[0, :, c].astype(jnp.float32)
        out = out + share[:, H + h:H + h + 1] * part[1, :, c].astype(jnp.float32)
        out_ref[:, c] = out.astype(out_ref.dtype)

    left(kv_send.at[0], got_kv.at[:, :, 0:(half - 1) * rows, :])
    left(q_send.at[0], got_q.at[0:most, :])
    left(o_send.at[0], att.at[0:most, :])
    left(l_send.at[0], lse_in.at[0:n - 1])


def shards(queries, fresh_keys, fresh_values, stale_keys, stale_values, patch_sizes):
    rows, columns = queries.shape
    n = lax.axis_size("seq")
    hd = columns // H
    half = n // 2
    held = H // half
    keys, lanes = half * rows, 128
    dma = pltpu.SemaphoreType.DMA
    kind = queries.dtype
    return pl.pallas_call(
        functools.partial(kernel, n),
        out_shape=pltpu.VMEM((rows, columns), kind),
        in_specs=[pl.BlockSpec(memory_space=pl.ANY)] * 6,
        out_specs=pl.BlockSpec(memory_space=pltpu.VMEM),
        scratch_shapes=[
            pltpu.VMEM((5, rows, columns), kind),
            pltpu.VMEM((n * rows, held * hd), kind),
            pltpu.VMEM((held, 4, keys, hd), kind),
            pltpu.VMEM((held, hd, 2 * keys), kind),
            pltpu.VMEM((n * rows, held * hd), kind),
            pltpu.VMEM((n * rows // lanes, held, lanes), jnp.float32),
            pltpu.VMEM((2, rows, columns), kind),
            pltpu.VMEM((n, held, lanes), jnp.float32),
            pltpu.VMEM((lanes, lanes), jnp.float32),
            pltpu.SMEM(patch_sizes.shape, patch_sizes.dtype),
            dma((2,)), dma((held,)), dma((n * rows // lanes,)), dma((1,)), dma((1,)),
            dma((1,)), dma((1,)), dma((1,)), dma((1,)),
            pltpu.SemaphoreType.REGULAR((n // 2,)),
        ],
        compiler_params=pltpu.CompilerParams(collective_id=0, has_side_effects=True),
    )(fresh_keys, stale_keys, fresh_values, stale_values, queries, patch_sizes)


def solution(mesh):
    spec = P(("groups", "seq"), None)
    body = shards if mesh.shape["seq"] == H else spread_shards
    return jax.shard_map(
        body, mesh=mesh, in_specs=(spec,) * 5 + (P("groups"),), out_specs=spec, check_vma=False)
```

```python
import functools

import jax
import jax.numpy as jnp
from jax import lax
from jax.experimental import pallas as pl
from jax.experimental.pallas import tpu as pltpu
from jax.sharding import PartitionSpec as P

H = 16
MESH = pl.DeviceIdType.MESH


def each(count, body):
    if count <= 32:
        for k in range(1, count):
            body(k)
    else:
        lax.fori_loop(1, count, lambda k, c: (body(k), c)[1], 0)


def flipped(me, k, count):
    if count & (count - 1):
        return lax.rem(me + k, count)
    peer, bit = 0, 1
    while bit < count:
        peer = peer + bit * lax.rem(me // bit + k // bit, 2)
        bit *= 2
    return peer


def spread_kernel(
    n, fk_ref, sk_ref, fv_ref, sv_ref, q_ref, sizes_ref, out_ref,
    stage, got_q, got_kv, att,
    load_sem, own_sem, send_sem, recv_sem, back_send, back_recv,
):
    rows, columns = q_ref.shape
    hd = columns // H
    me = lax.axis_index("seq")
    head = lax.rem(me, H)
    base = me - head
    keys = n * rows
    queries = H * rows

    loads = []
    for i, ref in enumerate((fk_ref, sk_ref, fv_ref, sv_ref, q_ref)):
        c = pltpu.make_async_copy(ref, stage.at[i], load_sem.at[i])
        c.start()
        loads.append(c)

    barrier = pltpu.get_barrier_semaphore()
    each(n, lambda k: pl.semaphore_signal(
        barrier, inc=1, device_id={"seq": flipped(me, k, n)}, device_id_type=MESH))
    pl.semaphore_wait(barrier, n - 1)

    def cols(h):
        return pl.ds(pl.multiple_of(h * hd, hd), hd)

    def at(p):
        return pl.ds(pl.multiple_of(p * rows, rows), rows)

    def views(phase, peer_head, source):
        if phase == 0:
            return stage.at[0:4, :, cols(peer_head)], got_kv.at[:, at(source), :]
        return stage.at[4, :, cols(peer_head)], got_q.at[at(lax.rem(source, H)), :]

    def remote(phase, peer, source, slot):
        src, dst = views(phase, lax.rem(peer, H), source)
        return pltpu.make_async_remote_copy(
            src_ref=src, dst_ref=dst,
            send_sem=send_sem.at[phase, slot], recv_sem=recv_sem.at[phase, slot],
            device_id={"seq": peer}, device_id_type=MESH)

    def own(phase):
        src, dst = views(phase, head, me)
        return pltpu.make_async_copy(src, dst, own_sem.at[phase])

    loads[4].wait()
    each(H, lambda k: remote(1, base + flipped(head, k, H), me, k).start())
    own(1).start()
    for i in range(4):
        loads[i].wait()
    each(n, lambda k: remote(0, flipped(me, k, n), me, k).start())
    own(0).start()

    ends, total = [], 0
    for p in range(sizes_ref.shape[0] - 1):
        total = total + sizes_ref[p]
        ends.append(total)

    block = 4 * rows
    scale = hd ** (-0.5)
    contract = (((1,), (1,)), ((), ()))

    def attend(b):
        at_b = pl.ds(pl.multiple_of(b * block, block), block)
        token = base * rows + b * block + lax.broadcasted_iota(jnp.int32, (block, 1), 0)
        limit = jnp.full((block, 1), keys, jnp.int32)
        for e in reversed(ends):
            limit = jnp.where(token < e, e, limit)
        fresh = lax.broadcasted_iota(jnp.int32, (block, keys), 1) < limit
        qb = got_q[at_b, :]
        sf = lax.dot_general(qb, got_kv[0], contract, preferred_element_type=jnp.float32)
        ss = lax.dot_general(qb, got_kv[1], contract, preferred_element_type=jnp.float32)
        s = jnp.where(fresh, sf, ss)
        w = jnp.exp((s - jnp.max(s, axis=1, keepdims=True)) * scale)
        den = jnp.sum(w, axis=1, keepdims=True)
        zero = jnp.zeros_like(w)
        wf = jnp.where(fresh, w, zero).astype(jnp.bfloat16)
        ws = jnp.where(fresh, zero, w).astype(jnp.bfloat16)
        num = jnp.dot(wf, got_kv[2], preferred_element_type=jnp.float32)
        num = num + jnp.dot(ws, got_kv[3], preferred_element_type=jnp.float32)
        att[at_b, :] = (num / den).astype(jnp.bfloat16)

    def back(slot):
        j = flipped(head, slot, H)
        return pltpu.make_async_remote_copy(
            src_ref=att.at[at(j), :], dst_ref=out_ref.at[:, cols(head)],
            send_sem=back_send.at[slot], recv_sem=back_recv.at[slot],
            device_id={"seq": base + j}, device_id_type=MESH)

    back_own = pltpu.make_async_copy(att.at[at(head), :], out_ref.at[:, cols(head)], own_sem.at[2])

    each(n, lambda k: remote(0, me, me, k).wait_recv())
    own(0).wait()
    for k in (2, 3, 1, 0):
        for slot in range(4 * k, 4 * k + 4):
            if slot:
                remote(1, me, me, slot).wait_recv()
            else:
                own(1).wait()
        attend(flipped(head // 4, k, H // 4))
        for slot in range(4 * k, 4 * k + 4):
            if slot:
                back(slot).start()
            else:
                back_own.start()

    each(n, lambda k: remote(0, me, me, k).wait_send())
    each(H, lambda k: remote(1, me, me, k).wait_send())
    for slot in range(1, H):
        back(slot).wait()
    back_own.wait()


def spread_shards(queries, fresh_keys, fresh_values, stale_keys, stale_values, patch_sizes):
    rows, columns = queries.shape
    n = lax.axis_size("seq")
    hd = columns // H
    keys, count = n * rows, H * rows
    dma = pltpu.SemaphoreType.DMA
    any_spec = pl.BlockSpec(memory_space=pl.ANY)
    return pl.pallas_call(
        functools.partial(spread_kernel, n),
        out_shape=pltpu.VMEM((rows, columns), queries.dtype),
        in_specs=[any_spec] * 5 + [pl.BlockSpec(memory_space=pltpu.SMEM)],
        out_specs=pl.BlockSpec(memory_space=pltpu.VMEM),
        scratch_shapes=[
            pltpu.VMEM((5, rows, columns), queries.dtype),
            pltpu.VMEM((count, hd), queries.dtype),
            pltpu.VMEM((4, keys, hd), queries.dtype),
            pltpu.VMEM((count, hd), queries.dtype),
            dma((5,)), dma((3,)), dma((2, n)), dma((2, n)), dma((H,)), dma((H,)),
        ],
        compiler_params=pltpu.CompilerParams(collective_id=0, has_side_effects=True),
    )(fresh_keys, stale_keys, fresh_values, stale_values, queries, patch_sizes)


def kernel(
    n, fk_ref, sk_ref, fv_ref, sv_ref, q_ref, sizes_hbm, out_ref,
    stage, got_q, got_kv, turned, att, lse_out, part, lse_in, mix, sizes_ref,
    load_sem, kv_recv, q_recv, o_recv, l_recv, kv_send, q_send, o_send, l_send, ready,
):
    rows, columns = q_ref.shape
    hd = columns // H
    me = lax.axis_index("seq")
    half = n // 2
    held = H // half
    keys = half * rows
    lanes = lse_in.shape[2]
    per = lanes // rows
    chips = n // 2

    for i, ref in enumerate((fk_ref, sk_ref, fv_ref, sv_ref, q_ref)):
        pltpu.make_async_copy(ref, stage.at[i], load_sem.at[0]).start()
    load_sizes = pltpu.make_async_copy(sizes_hbm, sizes_ref, load_sem.at[1])
    load_sizes.start()

    def signal(sem, peer):
        pl.semaphore_signal(sem, inc=1, device_id={"seq": peer}, device_id_type=MESH)

    chip = lax.div(me, 2)
    core = me - 2 * chip
    side = lax.div(me, half)
    place = chip - side * (chips // 2)
    upper = lax.rem(chip, 2) == 1
    buddy = 2 * chip + 1 - core

    def wave(c):
        return c // 2 + c % 2

    mine = lax.div(chip + 1, 2)
    barrier = pltpu.get_barrier_semaphore()
    signal(barrier, buddy)
    for t in range(1, chips):
        @pl.when(mine < wave(t))
        def _():
            signal(barrier, 2 * t)
            signal(barrier, 2 * t + 1)
    pl.semaphore_wait(barrier, jnp.maximum(4 * mine - 2, 0) + 1)
    for t in range(chips - 2, -1, -1):
        @pl.when(mine > wave(t))
        def _():
            signal(ready.at[chip], 2 * t)
            signal(ready.at[chip], 2 * t + 1)

    def cols(h, count=1):
        return pl.ds(pl.multiple_of(h * hd, hd), count * hd)

    def at(p, count=1):
        return pl.ds(pl.multiple_of(p * rows, rows), count * rows)

    def to(peer, src, dst, send, recv):
        return pltpu.make_async_remote_copy(
            src_ref=src, dst_ref=dst, send_sem=send, recv_sem=recv,
            device_id={"seq": peer}, device_id_type=MESH)

    local = me - side * half

    def kv_views(a, peer):
        return (stage.at[0:4, :, cols((peer - side * half) * held + a)], got_kv.at[a, :, at(local), :])

    def q_views(peer, base):
        return stage.at[4, :, cols((peer - base) * held, held)], got_q.at[at(me), :]

    def o_views(a, peer):
        return att.at[at(peer), a * hd:(a + 1) * hd], part.at[side, :, cols(local * held + a)]

    def l_views(peer):
        return lse_out.at[peer // per if isinstance(peer, int) else lax.div(peer, per)], lse_in.at[me]

    def send_kv(a, peer):
        to(peer, *kv_views(a, peer), kv_send.at[0], kv_recv.at[a]).start()

    def send_q(base, peer):
        to(peer, *q_views(peer, base), q_send.at[0], q_recv.at[lax.div(me, per)]).start()

    def send_o(a, peer):
        to(peer, *o_views(a, peer), o_send.at[0], o_recv.at[0]).start()

    def send_l(peer):
        to(peer, *l_views(peer), l_send.at[0], l_recv.at[0]).start()

    def arrived(sem, ref):
        to(me, ref, ref, sem, sem).wait_recv()

    def left(sem, ref):
        to(me, ref, ref, sem, sem).wait_send()

    def keep(src, dst):
        dst[...] = src[...]

    def cores(target, body):
        body(2 * target)
        body(2 * target + 1)

    def hear(target):
        pl.semaphore_wait(ready.at[target], 2)

    quad = chips // 2

    def nears(body):
        for e in range(quad - 1, 0, -1):
            pl.when(place >= e)(lambda: cores(chip - e, body))
            pl.when(place + e < quad)(lambda: cores(chip + e, body))

    arrived(load_sem.at[0], stage)
    head_a = functools.partial(send_kv, 0)
    head_a(buddy)
    for e in range(1, quad):
        there = place >= e
        pl.when(there & upper if e == 1 else there)(lambda: cores(chip - e, head_a))
    for e in range(1, quad):
        there = place + e < quad

        @pl.when(there & jnp.logical_not(upper) if e == 1 else there)
        def _():
            hear(chip + e)
            cores(chip + e, head_a)

        if e == 1:
            pl.when((place >= 1) & jnp.logical_not(upper))(lambda: cores(chip - 1, head_a))
        if e == 2:
            pl.when((place + 1 < quad) & upper)(lambda: cores(chip + 1, head_a))

    @pl.when(side == 1)
    def _():
        for t in range(quad):
            cores(t, functools.partial(send_q, 0))

    @pl.when(side == 0)
    def _():
        edge = chip == quad - 1
        far = functools.partial(send_q, half)
        for t in range(quad, chips):
            @pl.when(jnp.logical_not(edge) if t == quad else side == 0)
            def _():
                hear(t)
                cores(t, far)

            if t == quad + 1:
                pl.when(edge)(lambda: cores(quad, far))

    def send_near_q():
        near_q = functools.partial(send_q, side * half)
        near_q(buddy)
        nears(near_q)

    pl.when(side == 0)(send_near_q)
    for a in range(1, held):
        send_kv(a, buddy)
        nears(functools.partial(send_kv, a))
    pl.when(side == 1)(send_near_q)
    for a in range(held):
        keep(*kv_views(a, me))
    keep(*q_views(me, side * half))
    load_sizes.wait()

    ends, total = [], 0
    for p in range(sizes_ref.shape[0] - 1):
        total = total + sizes_ref[p]
        ends.append(total)

    scale = hd ** (-0.5) * 1.4426950408889634
    contract = (((1,), (1,)), ((), ()))

    def turn(a):
        turned[a, :, 0:keys] = got_kv[a, 2].T
        turned[a, :, keys:2 * keys] = got_kv[a, 3].T

    def attend(a, start, count):
        at_q = slice(start, start + count)
        token = start + lax.broadcasted_iota(jnp.int32, (1, count), 1)
        limit = jnp.full((1, count), 2 * keys, jnp.int32)
        for e in reversed(ends):
            limit = jnp.where(token < e, e, limit)
        fresh = lax.broadcasted_iota(jnp.int32, (keys, count), 0) < limit - side * keys
        both = got_kv[a, 0:2].reshape(2 * keys, hd)
        qb = got_q[at_q, a * hd:(a + 1) * hd]
        x = lax.dot_general(both, qb, contract, preferred_element_type=jnp.float32)
        x = jnp.where(fresh, x[:keys], x[keys:])
        top = jnp.max(x, axis=0, keepdims=True)
        w = jnp.exp2((x - top) * scale)
        den = jnp.sum(w, axis=0, keepdims=True)
        zero = jnp.zeros_like(w)
        wf = jnp.where(fresh, w, zero).astype(jnp.bfloat16)
        ws = jnp.where(fresh, zero, w).astype(jnp.bfloat16)
        num = jnp.dot(turned[a], jnp.concatenate([wf, ws], axis=0), preferred_element_type=jnp.float32)
        att[at_q, a * hd:(a + 1) * hd] = (num * (1.0 / den)).T.astype(jnp.bfloat16)
        lse = top * scale + jnp.log2(den)
        for b in range(count // lanes):
            lse_out[start // lanes + b, a:a + 1, :] = lse[:, b * lanes:(b + 1) * lanes]

    def give(a, planes, last):
        for p in planes:
            for j in range(p * per, (p + 1) * per):
                @pl.when(me != j)
                def _(j=j):
                    if last:
                        send_l(j)
                    send_o(a, j)

    def own(a, last):
        if last:
            keep(*l_views(me))
        keep(*o_views(a, me))

    def work(a, planes, mine, last=False):
        attend(a, planes[0] * lanes, len(planes) * lanes)
        give(a, planes, last)
        if mine:
            own(a, last)

    def wait_kv(a):
        arrived(kv_recv.at[a], got_kv.at[a, :, 0:(half - 1) * rows, :])
        turn(a)

    def wait_q(planes, mine):
        for p in planes:
            if mine:
                pl.when(lax.div(me, per) == p)(lambda p=p: arrived(q_recv.at[p], got_q.at[0:(per - 1) * rows, :]))
                pl.when(lax.div(me, per) != p)(lambda p=p: arrived(q_recv.at[p], got_q.at[0:per * rows, :]))
            else:
                arrived(q_recv.at[p], got_q.at[0:per * rows, :])

    planes = n // per
    low_planes, high_planes = range(planes // 2), range(planes // 2, planes)
    end = held - 1

    @pl.when(side == 0)
    def _():
        wait_kv(0)
        for p in high_planes:
            wait_q([p], False)
            work(0, [p], False)
        wait_q(low_planes, True)
        work(0, low_planes, True)
        for a in range(1, held):
            wait_kv(a)
            work(a, low_planes, True, a == end)
            work(a, high_planes, False, a == end)

    @pl.when(side == 1)
    def _():
        for a in range(held):
            wait_kv(a)
            if a == 0:
                wait_q(low_planes, False)
            work(a, low_planes, False, a == end)
        wait_q(high_planes, True)
        for a in range(held):
            work(a, high_planes, True, a == end)

    most = (n - 1) * rows
    arrived(o_recv.at[0], att.at[0:most, :])
    arrived(l_recv.at[0], lse_in.at[0:n - 1])
    low = lse_in[0:half].reshape(H, lanes)
    high = lse_in[half:n].reshape(H, lanes)
    top = jnp.maximum(low, high)
    low, high = jnp.exp2(low - top), jnp.exp2(high - top)
    total = low + high
    fill = jnp.zeros((lanes - 2 * H, lanes), jnp.float32)
    mix[...] = jnp.concatenate([low / total, high / total, fill], axis=0).T
    share = mix[at(lax.rem(me, per)), :]
    for h in range(H):
        c = slice(h * hd, (h + 1) * hd)
        out = share[:, h:h + 1] * part[0, :, c].astype(jnp.float32)
        out = out + share[:, H + h:H + h + 1] * part[1, :, c].astype(jnp.float32)
        out_ref[:, c] = out.astype(out_ref.dtype)

    left(kv_send.at[0], got_kv.at[:, :, 0:(half - 1) * rows, :])
    left(q_send.at[0], got_q.at[0:most, :])
    left(o_send.at[0], att.at[0:most, :])
    left(l_send.at[0], lse_in.at[0:n - 1])


def shards(queries, fresh_keys, fresh_values, stale_keys, stale_values, patch_sizes):
    rows, columns = queries.shape
    n = lax.axis_size("seq")
    hd = columns // H
    half = n // 2
    held = H // half
    keys, lanes = half * rows, 128
    dma = pltpu.SemaphoreType.DMA
    kind = queries.dtype
    return pl.pallas_call(
        functools.partial(kernel, n),
        out_shape=pltpu.VMEM((rows, columns), kind),
        in_specs=[pl.BlockSpec(memory_space=pl.ANY)] * 6,
        out_specs=pl.BlockSpec(memory_space=pltpu.VMEM),
        scratch_shapes=[
            pltpu.VMEM((5, rows, columns), kind),
            pltpu.VMEM((n * rows, held * hd), kind),
            pltpu.VMEM((held, 4, keys, hd), kind),
            pltpu.VMEM((held, hd, 2 * keys), kind),
            pltpu.VMEM((n * rows, held * hd), kind),
            pltpu.VMEM((n * rows // lanes, held, lanes), jnp.float32),
            pltpu.VMEM((2, rows, columns), kind),
            pltpu.VMEM((n, held, lanes), jnp.float32),
            pltpu.VMEM((lanes, lanes), jnp.float32),
            pltpu.SMEM(patch_sizes.shape, patch_sizes.dtype),
            dma((2,)), dma((held,)), dma((n * rows // lanes,)), dma((1,)), dma((1,)),
            dma((1,)), dma((1,)), dma((1,)), dma((1,)),
            pltpu.SemaphoreType.REGULAR((n // 2,)),
        ],
        compiler_params=pltpu.CompilerParams(collective_id=0, has_side_effects=True),
    )(fresh_keys, stale_keys, fresh_values, stale_values, queries, patch_sizes)


def solution(mesh):
    spec = P(("groups", "seq"), None)
    body = shards if mesh.shape["seq"] == H else spread_shards
    return jax.shard_map(
        body, mesh=mesh, in_specs=(spec,) * 5 + (P("groups"),), out_specs=spec, check_vma=False)
```

```python
import functools

import jax
import jax.numpy as jnp
from jax import lax
from jax.experimental import pallas as pl
from jax.experimental.pallas import tpu as pltpu
from jax.sharding import PartitionSpec as P

H = 16
MESH = pl.DeviceIdType.MESH


def each(count, body):
    if count <= 32:
        for k in range(1, count):
            body(k)
    else:
        lax.fori_loop(1, count, lambda k, c: (body(k), c)[1], 0)


def flipped(me, k, count):
    if count & (count - 1):
        return lax.rem(me + k, count)
    peer, bit = 0, 1
    while bit < count:
        peer = peer + bit * lax.rem(me // bit + k // bit, 2)
        bit *= 2
    return peer


def spread_kernel(
    n, fk_ref, sk_ref, fv_ref, sv_ref, q_ref, sizes_ref, out_ref,
    stage, got_q, got_kv, att,
    load_sem, own_sem, send_sem, recv_sem, back_send, back_recv,
):
    rows, columns = q_ref.shape
    hd = columns // H
    me = lax.axis_index("seq")
    head = lax.rem(me, H)
    base = me - head
    keys = n * rows
    queries = H * rows

    loads = []
    for i, ref in enumerate((fk_ref, sk_ref, fv_ref, sv_ref, q_ref)):
        c = pltpu.make_async_copy(ref, stage.at[i], load_sem.at[i])
        c.start()
        loads.append(c)

    barrier = pltpu.get_barrier_semaphore()
    each(n, lambda k: pl.semaphore_signal(
        barrier, inc=1, device_id={"seq": flipped(me, k, n)}, device_id_type=MESH))
    pl.semaphore_wait(barrier, n - 1)

    def cols(h):
        return pl.ds(pl.multiple_of(h * hd, hd), hd)

    def at(p):
        return pl.ds(pl.multiple_of(p * rows, rows), rows)

    def views(phase, peer_head, source):
        if phase == 0:
            return stage.at[0:4, :, cols(peer_head)], got_kv.at[:, at(source), :]
        return stage.at[4, :, cols(peer_head)], got_q.at[at(lax.rem(source, H)), :]

    def remote(phase, peer, source, slot):
        src, dst = views(phase, lax.rem(peer, H), source)
        return pltpu.make_async_remote_copy(
            src_ref=src, dst_ref=dst,
            send_sem=send_sem.at[phase, slot], recv_sem=recv_sem.at[phase, slot],
            device_id={"seq": peer}, device_id_type=MESH)

    def own(phase):
        src, dst = views(phase, head, me)
        return pltpu.make_async_copy(src, dst, own_sem.at[phase])

    loads[4].wait()
    each(H, lambda k: remote(1, base + flipped(head, k, H), me, k).start())
    own(1).start()
    for i in range(4):
        loads[i].wait()
    each(n, lambda k: remote(0, flipped(me, k, n), me, k).start())
    own(0).start()

    ends, total = [], 0
    for p in range(sizes_ref.shape[0] - 1):
        total = total + sizes_ref[p]
        ends.append(total)

    block = 4 * rows
    scale = hd ** (-0.5)
    contract = (((1,), (1,)), ((), ()))

    def attend(b):
        at_b = pl.ds(pl.multiple_of(b * block, block), block)
        token = base * rows + b * block + lax.broadcasted_iota(jnp.int32, (block, 1), 0)
        limit = jnp.full((block, 1), keys, jnp.int32)
        for e in reversed(ends):
            limit = jnp.where(token < e, e, limit)
        fresh = lax.broadcasted_iota(jnp.int32, (block, keys), 1) < limit
        qb = got_q[at_b, :]
        sf = lax.dot_general(qb, got_kv[0], contract, preferred_element_type=jnp.float32)
        ss = lax.dot_general(qb, got_kv[1], contract, preferred_element_type=jnp.float32)
        s = jnp.where(fresh, sf, ss)
        w = jnp.exp((s - jnp.max(s, axis=1, keepdims=True)) * scale)
        den = jnp.sum(w, axis=1, keepdims=True)
        zero = jnp.zeros_like(w)
        wf = jnp.where(fresh, w, zero).astype(jnp.bfloat16)
        ws = jnp.where(fresh, zero, w).astype(jnp.bfloat16)
        num = jnp.dot(wf, got_kv[2], preferred_element_type=jnp.float32)
        num = num + jnp.dot(ws, got_kv[3], preferred_element_type=jnp.float32)
        att[at_b, :] = (num / den).astype(jnp.bfloat16)

    def back(slot):
        j = flipped(head, slot, H)
        return pltpu.make_async_remote_copy(
            src_ref=att.at[at(j), :], dst_ref=out_ref.at[:, cols(head)],
            send_sem=back_send.at[slot], recv_sem=back_recv.at[slot],
            device_id={"seq": base + j}, device_id_type=MESH)

    back_own = pltpu.make_async_copy(att.at[at(head), :], out_ref.at[:, cols(head)], own_sem.at[2])

    each(n, lambda k: remote(0, me, me, k).wait_recv())
    own(0).wait()
    for k in (2, 3, 1, 0):
        for slot in range(4 * k, 4 * k + 4):
            if slot:
                remote(1, me, me, slot).wait_recv()
            else:
                own(1).wait()
        attend(flipped(head // 4, k, H // 4))
        for slot in range(4 * k, 4 * k + 4):
            if slot:
                back(slot).start()
            else:
                back_own.start()

    each(n, lambda k: remote(0, me, me, k).wait_send())
    each(H, lambda k: remote(1, me, me, k).wait_send())
    for slot in range(1, H):
        back(slot).wait()
    back_own.wait()


def spread_shards(queries, fresh_keys, fresh_values, stale_keys, stale_values, patch_sizes):
    rows, columns = queries.shape
    n = lax.axis_size("seq")
    hd = columns // H
    keys, count = n * rows, H * rows
    dma = pltpu.SemaphoreType.DMA
    any_spec = pl.BlockSpec(memory_space=pl.ANY)
    return pl.pallas_call(
        functools.partial(spread_kernel, n),
        out_shape=pltpu.VMEM((rows, columns), queries.dtype),
        in_specs=[any_spec] * 5 + [pl.BlockSpec(memory_space=pltpu.SMEM)],
        out_specs=pl.BlockSpec(memory_space=pltpu.VMEM),
        scratch_shapes=[
            pltpu.VMEM((5, rows, columns), queries.dtype),
            pltpu.VMEM((count, hd), queries.dtype),
            pltpu.VMEM((4, keys, hd), queries.dtype),
            pltpu.VMEM((count, hd), queries.dtype),
            dma((5,)), dma((3,)), dma((2, n)), dma((2, n)), dma((H,)), dma((H,)),
        ],
        compiler_params=pltpu.CompilerParams(collective_id=0, has_side_effects=True),
    )(fresh_keys, stale_keys, fresh_values, stale_values, queries, patch_sizes)


def kernel(
    n, fk_ref, sk_ref, fv_ref, sv_ref, q_ref, sizes_hbm, out_ref,
    stage, got_q, got_kv, turned, att, lse_out, part, lse_in, mix, sizes_ref,
    load_sem, kv_recv, q_recv, o_recv, l_recv, kv_send, q_send, o_send, l_send, ready,
):
    rows, columns = q_ref.shape
    hd = columns // H
    me = lax.axis_index("seq")
    half = n // 2
    held = H // half
    keys = half * rows
    lanes = lse_in.shape[2]
    per = lanes // rows
    chips = n // 2

    for i, ref in enumerate((fk_ref, sk_ref, fv_ref, sv_ref, q_ref)):
        for r in range(0, rows, 16):
            piece = pl.ds(r, min(16, rows))
            pltpu.make_async_copy(ref.at[piece, :], stage.at[i, piece, :], load_sem.at[i // 4]).start()
    load_sizes = pltpu.make_async_copy(sizes_hbm, sizes_ref, load_sem.at[2])
    load_sizes.start()

    def signal(sem, peer):
        pl.semaphore_signal(sem, inc=1, device_id={"seq": peer}, device_id_type=MESH)

    chip = lax.div(me, 2)
    core = me - 2 * chip
    side = lax.div(me, half)
    place = chip - side * (chips // 2)
    upper = lax.rem(chip, 2) == 1
    buddy = 2 * chip + 1 - core

    floor = lax.div(chip, 2)
    barrier = pltpu.get_barrier_semaphore()
    signal(barrier, buddy)

    def tell(sem, target):
        signal(sem, 2 * target)
        signal(sem, 2 * target + 1)

    for t in range(1, chips):
        later = floor < t // 2
        if t % 2:
            pl.when(later | ((chip < t) & jnp.logical_not(upper)))(functools.partial(tell, barrier, t))
        else:
            pl.when(later & jnp.logical_not(upper))(functools.partial(tell, barrier, t))
    pl.semaphore_wait(barrier, jnp.where(upper, 4 * floor + 3, 2 * floor + 1))
    for t in range(chips - 2, -1, -1):
        if t % 2:
            pl.when((chip > t) & upper)(functools.partial(tell, ready.at[chip], t))
        else:
            pl.when((floor > t // 2) | ((chip > t) & upper))(functools.partial(tell, ready.at[chip], t))

    def cols(h, count=1):
        return pl.ds(pl.multiple_of(h * hd, hd), count * hd)

    def at(p, count=1):
        return pl.ds(pl.multiple_of(p * rows, rows), count * rows)

    def to(peer, src, dst, send, recv):
        return pltpu.make_async_remote_copy(
            src_ref=src, dst_ref=dst, send_sem=send, recv_sem=recv,
            device_id={"seq": peer}, device_id_type=MESH)

    local = me - side * half

    def kv_views(a, peer):
        return (stage.at[0:4, :, cols((peer - side * half) * held + a)], got_kv.at[a, :, at(local), :])

    def q_views(peer, base):
        return stage.at[4, :, cols((peer - base) * held, held)], got_q.at[at(me), :]

    def o_views(a, peer):
        return att.at[at(peer), a * hd:(a + 1) * hd], part.at[side, :, cols(local * held + a)]

    def l_views(peer):
        return lse_out.at[peer // per if isinstance(peer, int) else lax.div(peer, per)], lse_in.at[me]

    def send_kv(a, peer):
        to(peer, *kv_views(a, peer), kv_send.at[0], kv_recv.at[a]).start()

    def send_q(base, peer):
        to(peer, *q_views(peer, base), q_send.at[0], q_recv.at[lax.div(me, per)]).start()

    def send_o(a, peer):
        to(peer, *o_views(a, peer), o_send.at[0], o_recv.at[a]).start()

    def send_l(peer):
        to(peer, *l_views(peer), l_send.at[0], l_recv.at[0]).start()

    def arrived(sem, ref):
        to(me, ref, ref, sem, sem).wait_recv()

    def left(sem, ref):
        to(me, ref, ref, sem, sem).wait_send()

    def keep(src, dst):
        dst[...] = src[...]

    def cores(target, body):
        body(2 * target)
        body(2 * target + 1)

    def hear(target):
        pl.semaphore_wait(ready.at[target], 2)

    quad = chips // 2

    first = side * quad
    across = 2 * first + quad - 1 - chip
    along = first + lax.rem(place + 2, quad)
    beside = chip + 1 - 2 * lax.rem(chip, 2)

    def nears(body):
        for target in (across, along, beside):
            cores(target, body)

    arrived(load_sem.at[0], stage.at[0:4])
    head_a = functools.partial(send_kv, 0)
    head_a(buddy)

    @pl.when(place == 0)
    def _():
        for target in (beside, along, across):
            hear(target)
            cores(target, head_a)

    @pl.when(place == 1)
    def _():
        cores(beside, head_a)
        hear(along)
        cores(across, head_a)
        cores(along, head_a)

    @pl.when(place == 2)
    def _():
        cores(along, head_a)
        hear(beside)
        cores(across, head_a)
        cores(beside, head_a)

    @pl.when(place == 3)
    def _():
        nears(head_a)

    arrived(load_sem.at[1], stage.at[4])

    @pl.when(side == 1)
    def _():
        for t in range(quad):
            cores(t, functools.partial(send_q, 0))

    @pl.when(side == 0)
    def _():
        far = functools.partial(send_q, half)
        for t in range(quad, chips, 2):
            @pl.when(jnp.logical_not(upper))
            def _():
                hear(t)
                cores(t, far)
                hear(t + 1)
                cores(t + 1, far)

            @pl.when(upper)
            def _():
                hear(t + 1)
                cores(t + 1, far)
                cores(t, far)

    def send_near_q():
        near_q = functools.partial(send_q, side * half)
        near_q(buddy)
        nears(near_q)

    pl.when(side == 0)(send_near_q)
    for a in range(1, held):
        send_kv(a, buddy)
        nears(functools.partial(send_kv, a))
    pl.when(side == 1)(send_near_q)
    for a in range(held):
        keep(*kv_views(a, me))
    keep(*q_views(me, side * half))
    load_sizes.wait()

    ends, total = [], 0
    for p in range(sizes_ref.shape[0] - 1):
        total = total + sizes_ref[p]
        ends.append(total)

    scale = hd ** (-0.5) * 1.4426950408889634
    contract = (((1,), (1,)), ((), ()))

    def turn(a):
        turned[a, :, 0:keys] = got_kv[a, 2].T
        turned[a, :, keys:2 * keys] = got_kv[a, 3].T

    def attend(a, start, count):
        at_q = slice(start, start + count)
        token = start + lax.broadcasted_iota(jnp.int32, (1, count), 1)
        limit = jnp.full((1, count), 2 * keys, jnp.int32)
        for e in reversed(ends):
            limit = jnp.where(token < e, e, limit)
        fresh = lax.broadcasted_iota(jnp.int32, (keys, count), 0) < limit - side * keys
        both = got_kv[a, 0:2].reshape(2 * keys, hd)
        qb = got_q[at_q, a * hd:(a + 1) * hd]
        x = lax.dot_general(both, qb, contract, preferred_element_type=jnp.float32)
        x = jnp.where(fresh, x[:keys], x[keys:])
        top = jnp.max(x, axis=0, keepdims=True)
        w = jnp.exp2((x - top) * scale)
        den = jnp.sum(w, axis=0, keepdims=True)
        zero = jnp.zeros_like(w)
        wf = jnp.where(fresh, w, zero).astype(jnp.bfloat16)
        ws = jnp.where(fresh, zero, w).astype(jnp.bfloat16)
        num = jnp.dot(turned[a], jnp.concatenate([wf, ws], axis=0), preferred_element_type=jnp.float32)
        att[at_q, a * hd:(a + 1) * hd] = (num * (1.0 / den)).T.astype(jnp.bfloat16)
        lse = top * scale + jnp.log2(den)
        for b in range(count // lanes):
            lse_out[start // lanes + b, a:a + 1, :] = lse[:, b * lanes:(b + 1) * lanes]

    def give(a, planes, last):
        for p in planes if planes[0] < n // per // 2 else reversed(planes):
            for j in range(p * per, (p + 1) * per):
                @pl.when(me != j)
                def _(j=j):
                    if last:
                        send_l(j)
                    send_o(a, j)

    def own(a, last):
        if last:
            keep(*l_views(me))
        keep(*o_views(a, me))

    def work(a, planes, mine, last=False):
        attend(a, planes[0] * lanes, len(planes) * lanes)
        give(a, planes, last)
        if mine:
            own(a, last)

    def wait_kv(a):
        arrived(kv_recv.at[a], got_kv.at[a, :, 0:(half - 1) * rows, :])
        turn(a)

    def wait_q(planes, mine):
        for p in planes:
            if mine:
                pl.when(lax.div(me, per) == p)(lambda p=p: arrived(q_recv.at[p], got_q.at[0:(per - 1) * rows, :]))
                pl.when(lax.div(me, per) != p)(lambda p=p: arrived(q_recv.at[p], got_q.at[0:per * rows, :]))
            else:
                arrived(q_recv.at[p], got_q.at[0:per * rows, :])

    planes = n // per
    low_planes, high_planes = range(planes // 2), range(planes // 2, planes)
    end = held - 1

    @pl.when(side == 0)
    def _():
        wait_kv(0)
        for p in high_planes:
            wait_q([p], False)
            work(0, [p], False)
        wait_q(low_planes, True)
        work(0, low_planes, True)
        for a in range(1, held):
            wait_kv(a)
            work(a, low_planes, True, a == end)
            work(a, high_planes, False, a == end)

    @pl.when(side == 1)
    def _():
        for a in range(held):
            wait_kv(a)
            if a == 0:
                wait_q(low_planes, False)
            work(a, low_planes, False, a == end)
        wait_q(high_planes, True)
        for a in range(held):
            work(a, high_planes, True, a == end)

    most = (n - 1) * rows
    arrived(l_recv.at[0], lse_in.at[0:n - 1])
    low = lse_in[0:half].reshape(H, lanes)
    high = lse_in[half:n].reshape(H, lanes)
    top = jnp.maximum(low, high)
    low, high = jnp.exp2(low - top), jnp.exp2(high - top)
    total = low + high
    fill = jnp.zeros((lanes - 2 * H, lanes), jnp.float32)
    mix[...] = jnp.concatenate([low / total, high / total, fill], axis=0).T
    share = mix[at(lax.rem(me, per)), :]
    for a in range(held):
        arrived(o_recv.at[a], att.at[0:most, 0:hd])
        for h in range(a, H, held):
            c = slice(h * hd, (h + 1) * hd)
            out = share[:, h:h + 1] * part[0, :, c].astype(jnp.float32)
            out = out + share[:, H + h:H + h + 1] * part[1, :, c].astype(jnp.float32)
            out_ref[:, c] = out.astype(out_ref.dtype)

    left(kv_send.at[0], got_kv.at[:, :, 0:(half - 1) * rows, :])
    left(q_send.at[0], got_q.at[0:most, :])
    left(o_send.at[0], att.at[0:most, :])
    left(l_send.at[0], lse_in.at[0:n - 1])


def shards(queries, fresh_keys, fresh_values, stale_keys, stale_values, patch_sizes):
    rows, columns = queries.shape
    n = lax.axis_size("seq")
    hd = columns // H
    half = n // 2
    held = H // half
    keys, lanes = half * rows, 128
    dma = pltpu.SemaphoreType.DMA
    kind = queries.dtype
    return pl.pallas_call(
        functools.partial(kernel, n),
        out_shape=pltpu.VMEM((rows, columns), kind),
        in_specs=[pl.BlockSpec(memory_space=pl.ANY)] * 6,
        out_specs=pl.BlockSpec(memory_space=pltpu.VMEM),
        scratch_shapes=[
            pltpu.VMEM((5, rows, columns), kind),
            pltpu.VMEM((n * rows, held * hd), kind),
            pltpu.VMEM((held, 4, keys, hd), kind),
            pltpu.VMEM((held, hd, 2 * keys), kind),
            pltpu.VMEM((n * rows, held * hd), kind),
            pltpu.VMEM((n * rows // lanes, held, lanes), jnp.float32),
            pltpu.VMEM((2, rows, columns), kind),
            pltpu.VMEM((n, held, lanes), jnp.float32),
            pltpu.VMEM((lanes, lanes), jnp.float32),
            pltpu.SMEM(patch_sizes.shape, patch_sizes.dtype),
            dma((3,)), dma((held,)), dma((n * rows // lanes,)), dma((held,)), dma((1,)),
            dma((1,)), dma((1,)), dma((1,)), dma((1,)),
            pltpu.SemaphoreType.REGULAR((n // 2,)),
        ],
        compiler_params=pltpu.CompilerParams(collective_id=0, has_side_effects=True),
    )(fresh_keys, stale_keys, fresh_values, stale_values, queries, patch_sizes)


def solution(mesh):
    spec = P(("groups", "seq"), None)
    body = shards if mesh.shape["seq"] == H else spread_shards
    return jax.shard_map(
        body, mesh=mesh, in_specs=(spec,) * 5 + (P("groups"),), out_specs=spec, check_vma=False)
```

```python
import functools

import jax
import jax.numpy as jnp
from jax import lax
from jax.experimental import pallas as pl
from jax.experimental.pallas import tpu as pltpu
from jax.sharding import PartitionSpec as P

H = 16
MESH = pl.DeviceIdType.MESH


def each(count, body):
    if count <= 32:
        for k in range(1, count):
            body(k)
    else:
        lax.fori_loop(1, count, lambda k, c: (body(k), c)[1], 0)


def flipped(me, k, count):
    if count & (count - 1):
        return lax.rem(me + k, count)
    peer, bit = 0, 1
    while bit < count:
        peer = peer + bit * lax.rem(me // bit + k // bit, 2)
        bit *= 2
    return peer


def spread_kernel(
    n, fk_ref, sk_ref, fv_ref, sv_ref, q_ref, sizes_ref, out_ref,
    stage, got_q, got_kv, att,
    load_sem, own_sem, send_sem, recv_sem, back_send, back_recv,
):
    rows, columns = q_ref.shape
    hd = columns // H
    me = lax.axis_index("seq")
    head = lax.rem(me, H)
    base = me - head
    keys = n * rows
    queries = H * rows

    loads = []
    for i, ref in enumerate((fk_ref, sk_ref, fv_ref, sv_ref, q_ref)):
        c = pltpu.make_async_copy(ref, stage.at[i], load_sem.at[i])
        c.start()
        loads.append(c)

    barrier = pltpu.get_barrier_semaphore()
    each(n, lambda k: pl.semaphore_signal(
        barrier, inc=1, device_id={"seq": flipped(me, k, n)}, device_id_type=MESH))
    pl.semaphore_wait(barrier, n - 1)

    def cols(h):
        return pl.ds(pl.multiple_of(h * hd, hd), hd)

    def at(p):
        return pl.ds(pl.multiple_of(p * rows, rows), rows)

    def views(phase, peer_head, source):
        if phase == 0:
            return stage.at[0:4, :, cols(peer_head)], got_kv.at[:, at(source), :]
        return stage.at[4, :, cols(peer_head)], got_q.at[at(lax.rem(source, H)), :]

    def remote(phase, peer, source, slot):
        src, dst = views(phase, lax.rem(peer, H), source)
        return pltpu.make_async_remote_copy(
            src_ref=src, dst_ref=dst,
            send_sem=send_sem.at[phase, slot], recv_sem=recv_sem.at[phase, slot],
            device_id={"seq": peer}, device_id_type=MESH)

    def own(phase):
        src, dst = views(phase, head, me)
        return pltpu.make_async_copy(src, dst, own_sem.at[phase])

    loads[4].wait()
    each(H, lambda k: remote(1, base + flipped(head, k, H), me, k).start())
    own(1).start()
    for i in range(4):
        loads[i].wait()
    each(n, lambda k: remote(0, flipped(me, k, n), me, k).start())
    own(0).start()

    ends, total = [], 0
    for p in range(sizes_ref.shape[0] - 1):
        total = total + sizes_ref[p]
        ends.append(total)

    block = 4 * rows
    scale = hd ** (-0.5)
    contract = (((1,), (1,)), ((), ()))

    def attend(b):
        at_b = pl.ds(pl.multiple_of(b * block, block), block)
        token = base * rows + b * block + lax.broadcasted_iota(jnp.int32, (block, 1), 0)
        limit = jnp.full((block, 1), keys, jnp.int32)
        for e in reversed(ends):
            limit = jnp.where(token < e, e, limit)
        fresh = lax.broadcasted_iota(jnp.int32, (block, keys), 1) < limit
        qb = got_q[at_b, :]
        sf = lax.dot_general(qb, got_kv[0], contract, preferred_element_type=jnp.float32)
        ss = lax.dot_general(qb, got_kv[1], contract, preferred_element_type=jnp.float32)
        s = jnp.where(fresh, sf, ss)
        w = jnp.exp((s - jnp.max(s, axis=1, keepdims=True)) * scale)
        den = jnp.sum(w, axis=1, keepdims=True)
        zero = jnp.zeros_like(w)
        wf = jnp.where(fresh, w, zero).astype(jnp.bfloat16)
        ws = jnp.where(fresh, zero, w).astype(jnp.bfloat16)
        num = jnp.dot(wf, got_kv[2], preferred_element_type=jnp.float32)
        num = num + jnp.dot(ws, got_kv[3], preferred_element_type=jnp.float32)
        att[at_b, :] = (num / den).astype(jnp.bfloat16)

    def back(slot):
        j = flipped(head, slot, H)
        return pltpu.make_async_remote_copy(
            src_ref=att.at[at(j), :], dst_ref=out_ref.at[:, cols(head)],
            send_sem=back_send.at[slot], recv_sem=back_recv.at[slot],
            device_id={"seq": base + j}, device_id_type=MESH)

    back_own = pltpu.make_async_copy(att.at[at(head), :], out_ref.at[:, cols(head)], own_sem.at[2])

    each(n, lambda k: remote(0, me, me, k).wait_recv())
    own(0).wait()
    for k in (2, 3, 1, 0):
        for slot in range(4 * k, 4 * k + 4):
            if slot:
                remote(1, me, me, slot).wait_recv()
            else:
                own(1).wait()
        attend(flipped(head // 4, k, H // 4))
        for slot in range(4 * k, 4 * k + 4):
            if slot:
                back(slot).start()
            else:
                back_own.start()

    each(n, lambda k: remote(0, me, me, k).wait_send())
    each(H, lambda k: remote(1, me, me, k).wait_send())
    for slot in range(1, H):
        back(slot).wait()
    back_own.wait()


def spread_shards(queries, fresh_keys, fresh_values, stale_keys, stale_values, patch_sizes):
    rows, columns = queries.shape
    n = lax.axis_size("seq")
    hd = columns // H
    keys, count = n * rows, H * rows
    dma = pltpu.SemaphoreType.DMA
    any_spec = pl.BlockSpec(memory_space=pl.ANY)
    return pl.pallas_call(
        functools.partial(spread_kernel, n),
        out_shape=pltpu.VMEM((rows, columns), queries.dtype),
        in_specs=[any_spec] * 5 + [pl.BlockSpec(memory_space=pltpu.SMEM)],
        out_specs=pl.BlockSpec(memory_space=pltpu.VMEM),
        scratch_shapes=[
            pltpu.VMEM((5, rows, columns), queries.dtype),
            pltpu.VMEM((count, hd), queries.dtype),
            pltpu.VMEM((4, keys, hd), queries.dtype),
            pltpu.VMEM((count, hd), queries.dtype),
            dma((5,)), dma((3,)), dma((2, n)), dma((2, n)), dma((H,)), dma((H,)),
        ],
        compiler_params=pltpu.CompilerParams(collective_id=0, has_side_effects=True),
    )(fresh_keys, stale_keys, fresh_values, stale_values, queries, patch_sizes)


def kernel(
    n, fk_ref, sk_ref, fv_ref, sv_ref, q_ref, sizes_hbm, out_ref,
    stage, got_q, got_kv, turned, att, lse_out, part, lse_in, mix, sizes_ref,
    load_sem, kv_recv, q_recv, o_recv, l_recv, kv_send, q_send, o_send, l_send, ready,
):
    rows, columns = q_ref.shape
    hd = columns // H
    me = lax.axis_index("seq")
    half = n // 2
    held = H // half
    keys = half * rows
    lanes = lse_in.shape[2]
    per = lanes // rows
    chips = n // 2

    for i, ref in enumerate((fk_ref, sk_ref, fv_ref, sv_ref, q_ref)):
        for r in range(0, rows, 16):
            piece = pl.ds(r, min(16, rows))
            pltpu.make_async_copy(ref.at[piece, :], stage.at[i, piece, :], load_sem.at[i // 4]).start()
    load_sizes = pltpu.make_async_copy(sizes_hbm, sizes_ref, load_sem.at[2])
    load_sizes.start()

    def signal(sem, peer):
        pl.semaphore_signal(sem, inc=1, device_id={"seq": peer}, device_id_type=MESH)

    chip = lax.div(me, 2)
    core = me - 2 * chip
    side = lax.div(me, half)
    place = chip - side * (chips // 2)
    upper = lax.rem(chip, 2) == 1
    buddy = 2 * chip + 1 - core

    floor = lax.div(chip, 2)
    barrier = pltpu.get_barrier_semaphore()
    signal(barrier, buddy)

    def tell(sem, target):
        signal(sem, 2 * target)
        signal(sem, 2 * target + 1)

    for t in range(1, chips):
        later = floor < t // 2
        if t % 2:
            pl.when(later | ((chip < t) & jnp.logical_not(upper)))(functools.partial(tell, barrier, t))
        else:
            pl.when(later & jnp.logical_not(upper))(functools.partial(tell, barrier, t))
    pl.semaphore_wait(barrier, jnp.where(upper, 4 * floor + 3, 2 * floor + 1))
    for t in range(chips - 2, -1, -1):
        if t % 2:
            pl.when((core == 1) & (chip > t) & upper)(functools.partial(tell, ready.at[chip], t))
        else:
            pl.when((core == 1) & ((floor > t // 2) | ((chip > t) & upper)))(functools.partial(tell, ready.at[chip], t))

    def cols(h, count=1):
        return pl.ds(pl.multiple_of(h * hd, hd), count * hd)

    def at(p, count=1):
        return pl.ds(pl.multiple_of(p * rows, rows), count * rows)

    def to(peer, src, dst, send, recv):
        return pltpu.make_async_remote_copy(
            src_ref=src, dst_ref=dst, send_sem=send, recv_sem=recv,
            device_id={"seq": peer}, device_id_type=MESH)

    local = me - side * half

    def kv_views(a, peer):
        return (stage.at[0:4, :, cols((peer - side * half) * held + a)], got_kv.at[a, :, at(local), :])

    def q_views(peer, base):
        return stage.at[4, :, cols((peer - base) * held, held)], got_q.at[at(me), :]

    def o_views(a, peer):
        return att.at[at(peer), a * hd:(a + 1) * hd], part.at[side, :, cols(local * held + a)]

    def l_views(peer):
        return lse_out.at[peer // per if isinstance(peer, int) else lax.div(peer, per)], lse_in.at[me]

    def send_kv(a, peer):
        to(peer, *kv_views(a, peer), kv_send.at[0], kv_recv.at[a]).start()

    def send_q(base, peer):
        to(peer, *q_views(peer, base), q_send.at[0], q_recv.at[lax.div(me, per)]).start()

    def send_o(a, peer):
        to(peer, *o_views(a, peer), o_send.at[0], o_recv.at[a]).start()

    def send_l(peer):
        to(peer, *l_views(peer), l_send.at[0], l_recv.at[0]).start()

    def arrived(sem, ref):
        to(me, ref, ref, sem, sem).wait_recv()

    def left(sem, ref):
        to(me, ref, ref, sem, sem).wait_send()

    def keep(src, dst):
        dst[...] = src[...]

    def cores(target, body):
        body(2 * target)
        body(2 * target + 1)

    def hear(target):
        pl.semaphore_wait(ready.at[target], 1)

    quad = chips // 2

    first = side * quad
    across = 2 * first + quad - 1 - chip
    along = first + lax.rem(place + 2, quad)
    beside = chip + 1 - 2 * lax.rem(chip, 2)

    def nears(body):
        swap = place == 1
        for target in (jnp.where(swap, along, across), jnp.where(swap, across, along), beside):
            cores(target, body)

    arrived(load_sem.at[0], stage.at[0:4])
    head_a = functools.partial(send_kv, 0)
    head_a(buddy)

    @pl.when(place == 0)
    def _():
        for target in (beside, along, across):
            hear(target)
            cores(target, head_a)

    @pl.when(place == 1)
    def _():
        cores(beside, head_a)
        hear(along)
        cores(across, head_a)
        cores(along, head_a)

    @pl.when(place == 2)
    def _():
        cores(along, head_a)
        hear(beside)
        cores(across, head_a)
        cores(beside, head_a)

    @pl.when(place == 3)
    def _():
        nears(head_a)

    arrived(load_sem.at[1], stage.at[4])

    last_plane = n // per - 1

    def send_one(a, peer):
        src = stage.at[4, :, cols(peer * held + a)]
        dst = got_q.at[at(me), a * hd:(a + 1) * hd]
        to(peer, src, dst, q_send.at[0], q_recv.at[last_plane + a]).start()

    @pl.when((side == 1) & (place < 2))
    def _():
        for t in range(quad):
            cores(t, functools.partial(send_q, 0))

    def send_low(a):
        for t in range(quad):
            cores(t, functools.partial(send_one, a))

    pl.when((side == 1) & (place >= 2))(functools.partial(send_low, 0))

    @pl.when(side == 0)
    def _():
        far = functools.partial(send_q, half)
        for t in range(quad, chips, 2):
            @pl.when(jnp.logical_not(upper))
            def _():
                hear(t)
                cores(t, far)
                hear(t + 1)
                cores(t + 1, far)

            @pl.when(upper)
            def _():
                hear(t + 1)
                cores(t + 1, far)
                cores(t, far)

    def send_near_q():
        near_q = functools.partial(send_q, side * half)
        near_q(buddy)
        nears(near_q)

    pl.when(side == 0)(send_near_q)
    for a in range(1, held):
        send_kv(a, buddy)
        nears(functools.partial(send_kv, a))
    for a in range(1, held):
        pl.when((side == 1) & (place >= 2))(functools.partial(send_low, a))
    pl.when(side == 1)(send_near_q)
    for a in range(held):
        keep(*kv_views(a, me))
    keep(*q_views(me, side * half))
    load_sizes.wait()

    ends, total = [], 0
    for p in range(sizes_ref.shape[0] - 1):
        total = total + sizes_ref[p]
        ends.append(total)

    scale = hd ** (-0.5) * 1.4426950408889634
    contract = (((1,), (1,)), ((), ()))

    def turn(a):
        turned[a, :, 0:keys] = got_kv[a, 2].T
        turned[a, :, keys:2 * keys] = got_kv[a, 3].T

    def attend(a, start, count):
        at_q = slice(start, start + count)
        token = start + lax.broadcasted_iota(jnp.int32, (1, count), 1)
        limit = jnp.full((1, count), 2 * keys, jnp.int32)
        for e in reversed(ends):
            limit = jnp.where(token < e, e, limit)
        fresh = lax.broadcasted_iota(jnp.int32, (keys, count), 0) < limit - side * keys
        both = got_kv[a, 0:2].reshape(2 * keys, hd)
        qb = got_q[at_q, a * hd:(a + 1) * hd]
        x = lax.dot_general(both, qb, contract, preferred_element_type=jnp.float32)
        x = jnp.where(fresh, x[:keys], x[keys:])
        top = jnp.max(x, axis=0, keepdims=True)
        w = jnp.exp2((x - top) * scale)
        den = jnp.sum(w, axis=0, keepdims=True)
        zero = jnp.zeros_like(w)
        wf = jnp.where(fresh, w, zero).astype(jnp.bfloat16)
        ws = jnp.where(fresh, zero, w).astype(jnp.bfloat16)
        num = jnp.dot(turned[a], jnp.concatenate([wf, ws], axis=0), preferred_element_type=jnp.float32)
        att[at_q, a * hd:(a + 1) * hd] = (num * (1.0 / den)).T.astype(jnp.bfloat16)
        lse = top * scale + jnp.log2(den)
        for b in range(count // lanes):
            lse_out[start // lanes + b, a:a + 1, :] = lse[:, b * lanes:(b + 1) * lanes]

    def give(a, planes, last):
        for p in planes if planes[0] < n // per // 2 else reversed(planes):
            for j in range(p * per, (p + 1) * per):
                @pl.when(me != j)
                def _(j=j):
                    if last:
                        send_l(j)
                    send_o(a, j)

    def own(a, last):
        if last:
            keep(*l_views(me))
        keep(*o_views(a, me))

    def work(a, planes, mine, last=False):
        attend(a, planes[0] * lanes, len(planes) * lanes)
        give(a, planes, last)
        if mine:
            own(a, last)

    def wait_kv(a):
        arrived(kv_recv.at[a], got_kv.at[a, :, 0:(half - 1) * rows, :])
        turn(a)

    def wait_q(planes, mine):
        for p in planes:
            if mine:
                pl.when(lax.div(me, per) == p)(lambda p=p: arrived(q_recv.at[p], got_q.at[0:(per - 1) * rows, :]))
                pl.when(lax.div(me, per) != p)(lambda p=p: arrived(q_recv.at[p], got_q.at[0:per * rows, :]))
            else:
                arrived(q_recv.at[p], got_q.at[0:per * rows, :])

    def wait_one(a):
        arrived(q_recv.at[last_plane + a], got_q.at[0:per * rows, 0:hd])

    planes = n // per
    low_planes, high_planes = range(planes // 2), range(planes // 2, planes)
    end = held - 1

    @pl.when(side == 0)
    def _():
        wait_kv(0)
        wait_q(high_planes[:1], False)
        work(0, high_planes[:1], False)
        wait_q(low_planes, True)
        work(0, low_planes, True)
        last = high_planes[-1:]
        wait_one(0)
        work(0, last, False)
        for a in range(1, held):
            wait_kv(a)
            work(a, low_planes, True, a == end)
            wait_one(a)
            work(a, high_planes, False, a == end)

    @pl.when(side == 1)
    def _():
        for a in range(held):
            wait_kv(a)
            if a == 0:
                wait_q(low_planes, False)
            work(a, low_planes, False, a == end)
        wait_q(high_planes, True)
        for a in range(held):
            work(a, high_planes, True, a == end)

    most = (n - 1) * rows
    arrived(l_recv.at[0], lse_in.at[0:n - 1])
    low = lse_in[0:half].reshape(H, lanes)
    high = lse_in[half:n].reshape(H, lanes)
    top = jnp.maximum(low, high)
    low, high = jnp.exp2(low - top), jnp.exp2(high - top)
    total = low + high
    fill = jnp.zeros((lanes - 2 * H, lanes), jnp.float32)
    mix[...] = jnp.concatenate([low / total, high / total, fill], axis=0).T
    share = mix[at(lax.rem(me, per)), :]
    for a in range(held):
        arrived(o_recv.at[a], att.at[0:most, 0:hd])
        for h in range(a, H, held):
            c = slice(h * hd, (h + 1) * hd)
            out = share[:, h:h + 1] * part[0, :, c].astype(jnp.float32)
            out = out + share[:, H + h:H + h + 1] * part[1, :, c].astype(jnp.float32)
            out_ref[:, c] = out.astype(out_ref.dtype)

    left(kv_send.at[0], got_kv.at[:, :, 0:(half - 1) * rows, :])
    left(q_send.at[0], got_q.at[0:most, :])
    left(o_send.at[0], att.at[0:most, :])
    left(l_send.at[0], lse_in.at[0:n - 1])


def shards(queries, fresh_keys, fresh_values, stale_keys, stale_values, patch_sizes):
    rows, columns = queries.shape
    n = lax.axis_size("seq")
    hd = columns // H
    half = n // 2
    held = H // half
    keys, lanes = half * rows, 128
    dma = pltpu.SemaphoreType.DMA
    kind = queries.dtype
    return pl.pallas_call(
        functools.partial(kernel, n),
        out_shape=pltpu.VMEM((rows, columns), kind),
        in_specs=[pl.BlockSpec(memory_space=pl.ANY)] * 6,
        out_specs=pl.BlockSpec(memory_space=pltpu.VMEM),
        scratch_shapes=[
            pltpu.VMEM((5, rows, columns), kind),
            pltpu.VMEM((n * rows, held * hd), kind),
            pltpu.VMEM((held, 4, keys, hd), kind),
            pltpu.VMEM((held, hd, 2 * keys), kind),
            pltpu.VMEM((n * rows, held * hd), kind),
            pltpu.VMEM((n * rows // lanes, held, lanes), jnp.float32),
            pltpu.VMEM((2, rows, columns), kind),
            pltpu.VMEM((n, held, lanes), jnp.float32),
            pltpu.VMEM((lanes, lanes), jnp.float32),
            pltpu.SMEM(patch_sizes.shape, patch_sizes.dtype),
            dma((3,)), dma((held,)), dma((n * rows // lanes + held - 1,)), dma((held,)), dma((1,)),
            dma((1,)), dma((1,)), dma((1,)), dma((1,)),
            pltpu.SemaphoreType.REGULAR((n // 2,)),
        ],
        compiler_params=pltpu.CompilerParams(collective_id=0, has_side_effects=True),
    )(fresh_keys, stale_keys, fresh_values, stale_values, queries, patch_sizes)


def solution(mesh):
    spec = P(("groups", "seq"), None)
    body = shards if mesh.shape["seq"] == H else spread_shards
    return jax.shard_map(
        body, mesh=mesh, in_specs=(spec,) * 5 + (P("groups"),), out_specs=spec, check_vma=False)
```

```python
import functools

import jax
import jax.numpy as jnp
from jax import lax
from jax.experimental import pallas as pl
from jax.experimental.pallas import tpu as pltpu
from jax.sharding import PartitionSpec as P

H = 16
MESH = pl.DeviceIdType.MESH


def each(count, body):
    if count <= 32:
        for k in range(1, count):
            body(k)
    else:
        lax.fori_loop(1, count, lambda k, c: (body(k), c)[1], 0)


def flipped(me, k, count):
    if count & (count - 1):
        return lax.rem(me + k, count)
    peer, bit = 0, 1
    while bit < count:
        peer = peer + bit * lax.rem(me // bit + k // bit, 2)
        bit *= 2
    return peer


def spread_kernel(
    n, fk_ref, sk_ref, fv_ref, sv_ref, q_ref, sizes_ref, out_ref,
    stage, got_q, got_kv, att,
    load_sem, own_sem, send_sem, recv_sem, back_send, back_recv,
):
    rows, columns = q_ref.shape
    hd = columns // H
    me = lax.axis_index("seq")
    head = lax.rem(me, H)
    base = me - head
    keys = n * rows
    queries = H * rows

    loads = []
    for i, ref in enumerate((fk_ref, sk_ref, fv_ref, sv_ref, q_ref)):
        c = pltpu.make_async_copy(ref, stage.at[i], load_sem.at[i])
        c.start()
        loads.append(c)

    barrier = pltpu.get_barrier_semaphore()
    each(n, lambda k: pl.semaphore_signal(
        barrier, inc=1, device_id={"seq": flipped(me, k, n)}, device_id_type=MESH))
    pl.semaphore_wait(barrier, n - 1)

    def cols(h):
        return pl.ds(pl.multiple_of(h * hd, hd), hd)

    def at(p):
        return pl.ds(pl.multiple_of(p * rows, rows), rows)

    def views(phase, peer_head, source):
        if phase == 0:
            return stage.at[0:4, :, cols(peer_head)], got_kv.at[:, at(source), :]
        return stage.at[4, :, cols(peer_head)], got_q.at[at(lax.rem(source, H)), :]

    def remote(phase, peer, source, slot):
        src, dst = views(phase, lax.rem(peer, H), source)
        return pltpu.make_async_remote_copy(
            src_ref=src, dst_ref=dst,
            send_sem=send_sem.at[phase, slot], recv_sem=recv_sem.at[phase, slot],
            device_id={"seq": peer}, device_id_type=MESH)

    def own(phase):
        src, dst = views(phase, head, me)
        return pltpu.make_async_copy(src, dst, own_sem.at[phase])

    loads[4].wait()
    each(H, lambda k: remote(1, base + flipped(head, k, H), me, k).start())
    own(1).start()
    for i in range(4):
        loads[i].wait()
    each(n, lambda k: remote(0, flipped(me, k, n), me, k).start())
    own(0).start()

    ends, total = [], 0
    for p in range(sizes_ref.shape[0] - 1):
        total = total + sizes_ref[p]
        ends.append(total)

    block = 4 * rows
    scale = hd ** (-0.5)
    contract = (((1,), (1,)), ((), ()))

    def attend(b):
        at_b = pl.ds(pl.multiple_of(b * block, block), block)
        token = base * rows + b * block + lax.broadcasted_iota(jnp.int32, (block, 1), 0)
        limit = jnp.full((block, 1), keys, jnp.int32)
        for e in reversed(ends):
            limit = jnp.where(token < e, e, limit)
        fresh = lax.broadcasted_iota(jnp.int32, (block, keys), 1) < limit
        qb = got_q[at_b, :]
        sf = lax.dot_general(qb, got_kv[0], contract, preferred_element_type=jnp.float32)
        ss = lax.dot_general(qb, got_kv[1], contract, preferred_element_type=jnp.float32)
        s = jnp.where(fresh, sf, ss)
        w = jnp.exp((s - jnp.max(s, axis=1, keepdims=True)) * scale)
        den = jnp.sum(w, axis=1, keepdims=True)
        zero = jnp.zeros_like(w)
        wf = jnp.where(fresh, w, zero).astype(jnp.bfloat16)
        ws = jnp.where(fresh, zero, w).astype(jnp.bfloat16)
        num = jnp.dot(wf, got_kv[2], preferred_element_type=jnp.float32)
        num = num + jnp.dot(ws, got_kv[3], preferred_element_type=jnp.float32)
        att[at_b, :] = (num / den).astype(jnp.bfloat16)

    def back(slot):
        j = flipped(head, slot, H)
        return pltpu.make_async_remote_copy(
            src_ref=att.at[at(j), :], dst_ref=out_ref.at[:, cols(head)],
            send_sem=back_send.at[slot], recv_sem=back_recv.at[slot],
            device_id={"seq": base + j}, device_id_type=MESH)

    back_own = pltpu.make_async_copy(att.at[at(head), :], out_ref.at[:, cols(head)], own_sem.at[2])

    each(n, lambda k: remote(0, me, me, k).wait_recv())
    own(0).wait()
    for k in (2, 3, 1, 0):
        for slot in range(4 * k, 4 * k + 4):
            if slot:
                remote(1, me, me, slot).wait_recv()
            else:
                own(1).wait()
        attend(flipped(head // 4, k, H // 4))
        for slot in range(4 * k, 4 * k + 4):
            if slot:
                back(slot).start()
            else:
                back_own.start()

    each(n, lambda k: remote(0, me, me, k).wait_send())
    each(H, lambda k: remote(1, me, me, k).wait_send())
    for slot in range(1, H):
        back(slot).wait()
    back_own.wait()


def spread_shards(queries, fresh_keys, fresh_values, stale_keys, stale_values, patch_sizes):
    rows, columns = queries.shape
    n = lax.axis_size("seq")
    hd = columns // H
    keys, count = n * rows, H * rows
    dma = pltpu.SemaphoreType.DMA
    any_spec = pl.BlockSpec(memory_space=pl.ANY)
    return pl.pallas_call(
        functools.partial(spread_kernel, n),
        out_shape=pltpu.VMEM((rows, columns), queries.dtype),
        in_specs=[any_spec] * 5 + [pl.BlockSpec(memory_space=pltpu.SMEM)],
        out_specs=pl.BlockSpec(memory_space=pltpu.VMEM),
        scratch_shapes=[
            pltpu.VMEM((5, rows, columns), queries.dtype),
            pltpu.VMEM((count, hd), queries.dtype),
            pltpu.VMEM((4, keys, hd), queries.dtype),
            pltpu.VMEM((count, hd), queries.dtype),
            dma((5,)), dma((3,)), dma((2, n)), dma((2, n)), dma((H,)), dma((H,)),
        ],
        compiler_params=pltpu.CompilerParams(collective_id=0, has_side_effects=True),
    )(fresh_keys, stale_keys, fresh_values, stale_values, queries, patch_sizes)


def kernel(
    n, fk_ref, sk_ref, fv_ref, sv_ref, q_ref, sizes_hbm, out_ref,
    stage, got_q, got_kv, turned, att, lse_out, part, lse_in, mix, sizes_ref,
    load_sem, kv_recv, q_recv, o_recv, l_recv, kv_send, q_send, o_send, l_send, ready,
):
    rows, columns = q_ref.shape
    hd = columns // H
    me = lax.axis_index("seq")
    half = n // 2
    held = H // half
    keys = half * rows
    lanes = lse_in.shape[2]
    per = lanes // rows
    chips = n // 2

    for i, ref in enumerate((fk_ref, sk_ref, fv_ref, sv_ref, q_ref)):
        for r in range(0, rows, 16):
            piece = pl.ds(r, min(16, rows))
            pltpu.make_async_copy(ref.at[piece, :], stage.at[i, piece, :], load_sem.at[i // 4]).start()
    load_sizes = pltpu.make_async_copy(sizes_hbm, sizes_ref, load_sem.at[2])
    load_sizes.start()

    def signal(sem, peer):
        pl.semaphore_signal(sem, inc=1, device_id={"seq": peer}, device_id_type=MESH)

    chip = lax.div(me, 2)
    core = me - 2 * chip
    side = lax.div(me, half)
    place = chip - side * (chips // 2)
    upper = lax.rem(chip, 2) == 1
    buddy = 2 * chip + 1 - core

    floor = lax.div(chip, 2)
    barrier = pltpu.get_barrier_semaphore()
    signal(barrier, buddy)

    def tell(sem, target):
        signal(sem, 2 * target)
        signal(sem, 2 * target + 1)

    for t in range(1, chips):
        later = floor < t // 2
        if t % 2:
            pl.when(later | ((chip < t) & jnp.logical_not(upper)))(functools.partial(tell, barrier, t))
        else:
            pl.when(later & jnp.logical_not(upper))(functools.partial(tell, barrier, t))
    pl.semaphore_wait(barrier, jnp.where(upper, 4 * floor + 3, 2 * floor + 1))
    for t in range(chips - 2, -1, -1):
        if t % 2:
            pl.when((core == 1) & (chip > t) & upper)(functools.partial(tell, ready.at[chip], t))
        else:
            pl.when((core == 1) & ((floor > t // 2) | ((chip > t) & upper)))(functools.partial(tell, ready.at[chip], t))

    def cols(h, count=1):
        return pl.ds(pl.multiple_of(h * hd, hd), count * hd)

    def at(p, count=1):
        return pl.ds(pl.multiple_of(p * rows, rows), count * rows)

    def to(peer, src, dst, send, recv):
        return pltpu.make_async_remote_copy(
            src_ref=src, dst_ref=dst, send_sem=send, recv_sem=recv,
            device_id={"seq": peer}, device_id_type=MESH)

    local = me - side * half

    def kv_views(a, peer):
        return (stage.at[0:4, :, cols((peer - side * half) * held + a)], got_kv.at[a, :, at(local), :])

    def q_views(peer, base):
        return stage.at[4, :, cols((peer - base) * held, held)], got_q.at[at(me), :]

    def o_views(a, peer):
        return att.at[at(peer), a * hd:(a + 1) * hd], part.at[side, :, cols(local * held + a)]

    def l_views(peer):
        return lse_out.at[peer // per if isinstance(peer, int) else lax.div(peer, per)], lse_in.at[me]

    def send_kv(a, peer):
        to(peer, *kv_views(a, peer), kv_send.at[0], kv_recv.at[a]).start()

    def send_q(base, peer):
        to(peer, *q_views(peer, base), q_send.at[0], q_recv.at[lax.div(me, per)]).start()

    def send_o(a, peer):
        to(peer, *o_views(a, peer), o_send.at[0], o_recv.at[a]).start()

    def send_l(peer):
        to(peer, *l_views(peer), l_send.at[0], l_recv.at[0]).start()

    def arrived(sem, ref):
        to(me, ref, ref, sem, sem).wait_recv()

    def left(sem, ref):
        to(me, ref, ref, sem, sem).wait_send()

    def keep(src, dst):
        dst[...] = src[...]

    def cores(target, body):
        body(2 * target)
        body(2 * target + 1)

    def hear(target):
        pl.semaphore_wait(ready.at[target], 1)

    quad = chips // 2

    first = side * quad
    across = 2 * first + quad - 1 - chip
    along = first + lax.rem(place + 2, quad)
    beside = chip + 1 - 2 * lax.rem(chip, 2)

    def nears(body):
        swap = place == 1
        for target in (jnp.where(swap, along, across), jnp.where(swap, across, along), beside):
            cores(target, body)

    arrived(load_sem.at[0], stage.at[0:4])
    head_a = functools.partial(send_kv, 0)
    head_a(buddy)

    @pl.when(place == 0)
    def _():
        for target in (beside, along, across):
            hear(target)
            cores(target, head_a)

    @pl.when(place == 1)
    def _():
        cores(beside, head_a)
        hear(along)
        cores(across, head_a)
        cores(along, head_a)

    @pl.when(place == 2)
    def _():
        cores(along, head_a)
        hear(beside)
        cores(across, head_a)
        cores(beside, head_a)

    @pl.when(place == 3)
    def _():
        nears(head_a)

    arrived(load_sem.at[1], stage.at[4])

    last_plane = n // per - 1

    def send_one(a, peer):
        src = stage.at[4, :, cols(peer * held + a)]
        dst = got_q.at[at(me), a * hd:(a + 1) * hd]
        to(peer, src, dst, q_send.at[0], q_recv.at[last_plane + a]).start()

    @pl.when((side == 1) & (place < 2))
    def _():
        for t in range(quad):
            cores(t, functools.partial(send_q, 0))

    def send_low(a):
        for t in range(quad):
            cores(t, functools.partial(send_one, a))

    pl.when((side == 1) & (place >= 2))(functools.partial(send_low, 0))

    @pl.when(side == 0)
    def _():
        far = functools.partial(send_q, half)
        for t in range(quad, chips, 2):
            now = place < (2 if t + 2 == chips else quad)

            @pl.when(jnp.logical_not(upper))
            def _():
                hear(t)
                pl.when(now)(lambda: cores(t, far))
                hear(t + 1)
                pl.when(now)(lambda: cores(t + 1, far))

            @pl.when(upper)
            def _():
                hear(t + 1)

                @pl.when(now)
                def _():
                    cores(t + 1, far)
                    cores(t, far)

    def send_top_q():
        for t in (chips - 2, chips - 1):
            cores(t, functools.partial(send_q, half))

    def send_near_q():
        near_q = functools.partial(send_q, side * half)
        near_q(buddy)
        nears(near_q)

    pl.when(side == 0)(send_near_q)
    for a in range(1, held):
        send_kv(a, buddy)
        nears(functools.partial(send_kv, a))
    for a in range(1, held):
        pl.when((side == 1) & (place >= 2))(functools.partial(send_low, a))
    pl.when(side == 1)(send_near_q)
    for a in range(held):
        keep(*kv_views(a, me))
    keep(*q_views(me, side * half))
    load_sizes.wait()

    ends, total = [], 0
    for p in range(sizes_ref.shape[0] - 1):
        total = total + sizes_ref[p]
        ends.append(total)

    scale = hd ** (-0.5) * 1.4426950408889634
    contract = (((1,), (1,)), ((), ()))

    def turn(a):
        turned[a, :, 0:keys] = got_kv[a, 2].T
        turned[a, :, keys:2 * keys] = got_kv[a, 3].T

    def attend(a, start, count):
        at_q = slice(start, start + count)
        token = start + lax.broadcasted_iota(jnp.int32, (1, count), 1)
        limit = jnp.full((1, count), 2 * keys, jnp.int32)
        for e in reversed(ends):
            limit = jnp.where(token < e, e, limit)
        fresh = lax.broadcasted_iota(jnp.int32, (keys, count), 0) < limit - side * keys
        both = got_kv[a, 0:2].reshape(2 * keys, hd)
        qb = got_q[at_q, a * hd:(a + 1) * hd]
        x = lax.dot_general(both, qb, contract, preferred_element_type=jnp.float32)
        x = jnp.where(fresh, x[:keys], x[keys:])
        top = jnp.max(x, axis=0, keepdims=True)
        w = jnp.exp2((x - top) * scale)
        den = jnp.sum(w, axis=0, keepdims=True)
        zero = jnp.zeros_like(w)
        wf = jnp.where(fresh, w, zero).astype(jnp.bfloat16)
        ws = jnp.where(fresh, zero, w).astype(jnp.bfloat16)
        num = jnp.dot(turned[a], jnp.concatenate([wf, ws], axis=0), preferred_element_type=jnp.float32)
        att[at_q, a * hd:(a + 1) * hd] = (num * (1.0 / den)).T.astype(jnp.bfloat16)
        lse = top * scale + jnp.log2(den)
        for b in range(count // lanes):
            lse_out[start // lanes + b, a:a + 1, :] = lse[:, b * lanes:(b + 1) * lanes]

    def give(a, planes, last):
        for p in planes if planes[0] < n // per // 2 else reversed(planes):
            for j in range(p * per, (p + 1) * per):
                @pl.when(me != j)
                def _(j=j):
                    if last:
                        send_l(j)
                    send_o(a, j)

    def own(a, last):
        if last:
            keep(*l_views(me))
        keep(*o_views(a, me))

    def work(a, planes, mine, last=False):
        attend(a, planes[0] * lanes, len(planes) * lanes)
        give(a, planes, last)
        if mine:
            own(a, last)

    def wait_kv(a):
        arrived(kv_recv.at[a], got_kv.at[a, :, 0:(half - 1) * rows, :])
        turn(a)

    def wait_q(planes, mine):
        for p in planes:
            if mine:
                pl.when(lax.div(me, per) == p)(lambda p=p: arrived(q_recv.at[p], got_q.at[0:(per - 1) * rows, :]))
                pl.when(lax.div(me, per) != p)(lambda p=p: arrived(q_recv.at[p], got_q.at[0:per * rows, :]))
            else:
                arrived(q_recv.at[p], got_q.at[0:per * rows, :])

    def wait_one(a):
        arrived(q_recv.at[last_plane + a], got_q.at[0:per * rows, 0:hd])

    planes = n // per
    low_planes, high_planes = range(planes // 2), range(planes // 2, planes)
    end = held - 1

    @pl.when(side == 0)
    def _():
        wait_kv(0)
        pl.when(place >= 2)(send_top_q)
        wait_q(high_planes[:1], False)
        work(0, high_planes[:1], False)
        wait_q(low_planes, True)
        work(0, low_planes, True)
        last = high_planes[-1:]
        wait_one(0)
        work(0, last, False)
        for a in range(1, held):
            wait_kv(a)
            work(a, low_planes, True, a == end)
            wait_one(a)
            work(a, high_planes, False, a == end)

    @pl.when(side == 1)
    def _():
        for p in low_planes:
            for a in range(held):
                if p == 0:
                    wait_kv(a)
                if a == 0:
                    wait_q([p], False)
                work(a, [p], False, a == end)
        wait_q(high_planes, True)
        for a in range(held):
            work(a, high_planes, True, a == end)

    most = (n - 1) * rows
    arrived(l_recv.at[0], lse_in.at[0:n - 1])
    low = lse_in[0:half].reshape(H, lanes)
    high = lse_in[half:n].reshape(H, lanes)
    top = jnp.maximum(low, high)
    low, high = jnp.exp2(low - top), jnp.exp2(high - top)
    total = low + high
    fill = jnp.zeros((lanes - 2 * H, lanes), jnp.float32)
    mix[...] = jnp.concatenate([low / total, high / total, fill], axis=0).T
    share = mix[at(lax.rem(me, per)), :]
    for a in range(held):
        arrived(o_recv.at[a], att.at[0:most, 0:hd])
        for h in range(a, H, held):
            c = slice(h * hd, (h + 1) * hd)
            out = share[:, h:h + 1] * part[0, :, c].astype(jnp.float32)
            out = out + share[:, H + h:H + h + 1] * part[1, :, c].astype(jnp.float32)
            out_ref[:, c] = out.astype(out_ref.dtype)

    left(kv_send.at[0], got_kv.at[:, :, 0:(half - 1) * rows, :])
    left(q_send.at[0], got_q.at[0:most, :])
    left(o_send.at[0], att.at[0:most, :])
    left(l_send.at[0], lse_in.at[0:n - 1])


def shards(queries, fresh_keys, fresh_values, stale_keys, stale_values, patch_sizes):
    rows, columns = queries.shape
    n = lax.axis_size("seq")
    hd = columns // H
    half = n // 2
    held = H // half
    keys, lanes = half * rows, 128
    dma = pltpu.SemaphoreType.DMA
    kind = queries.dtype
    return pl.pallas_call(
        functools.partial(kernel, n),
        out_shape=pltpu.VMEM((rows, columns), kind),
        in_specs=[pl.BlockSpec(memory_space=pl.ANY)] * 6,
        out_specs=pl.BlockSpec(memory_space=pltpu.VMEM),
        scratch_shapes=[
            pltpu.VMEM((5, rows, columns), kind),
            pltpu.VMEM((n * rows, held * hd), kind),
            pltpu.VMEM((held, 4, keys, hd), kind),
            pltpu.VMEM((held, hd, 2 * keys), kind),
            pltpu.VMEM((n * rows, held * hd), kind),
            pltpu.VMEM((n * rows // lanes, held, lanes), jnp.float32),
            pltpu.VMEM((2, rows, columns), kind),
            pltpu.VMEM((n, held, lanes), jnp.float32),
            pltpu.VMEM((lanes, lanes), jnp.float32),
            pltpu.SMEM(patch_sizes.shape, patch_sizes.dtype),
            dma((3,)), dma((held,)), dma((n * rows // lanes + held - 1,)), dma((held,)), dma((1,)),
            dma((1,)), dma((1,)), dma((1,)), dma((1,)),
            pltpu.SemaphoreType.REGULAR((n // 2,)),
        ],
        compiler_params=pltpu.CompilerParams(collective_id=0, has_side_effects=True),
    )(fresh_keys, stale_keys, fresh_values, stale_values, queries, patch_sizes)


def solution(mesh):
    spec = P(("groups", "seq"), None)
    body = shards if mesh.shape["seq"] == H else spread_shards
    return jax.shard_map(
        body, mesh=mesh, in_specs=(spec,) * 5 + (P("groups"),), out_specs=spec, check_vma=False)
```

```python
import functools

import jax
import jax.numpy as jnp
from jax import lax
from jax.experimental import pallas as pl
from jax.experimental.pallas import tpu as pltpu
from jax.sharding import PartitionSpec as P

H = 16
MESH = pl.DeviceIdType.MESH


def each(count, body):
    if count <= 32:
        for k in range(1, count):
            body(k)
    else:
        lax.fori_loop(1, count, lambda k, c: (body(k), c)[1], 0)


def flipped(me, k, count):
    if count & (count - 1):
        return lax.rem(me + k, count)
    peer, bit = 0, 1
    while bit < count:
        peer = peer + bit * lax.rem(me // bit + k // bit, 2)
        bit *= 2
    return peer


def spread_kernel(
    n, fk_ref, sk_ref, fv_ref, sv_ref, q_ref, sizes_ref, out_ref,
    stage, got_q, got_kv, att,
    load_sem, own_sem, send_sem, recv_sem, back_send, back_recv,
):
    rows, columns = q_ref.shape
    hd = columns // H
    me = lax.axis_index("seq")
    head = lax.rem(me, H)
    base = me - head
    keys = n * rows
    queries = H * rows

    loads = []
    for i, ref in enumerate((fk_ref, sk_ref, fv_ref, sv_ref, q_ref)):
        c = pltpu.make_async_copy(ref, stage.at[i], load_sem.at[i])
        c.start()
        loads.append(c)

    barrier = pltpu.get_barrier_semaphore()
    each(n, lambda k: pl.semaphore_signal(
        barrier, inc=1, device_id={"seq": flipped(me, k, n)}, device_id_type=MESH))
    pl.semaphore_wait(barrier, n - 1)

    def cols(h):
        return pl.ds(pl.multiple_of(h * hd, hd), hd)

    def at(p):
        return pl.ds(pl.multiple_of(p * rows, rows), rows)

    def views(phase, peer_head, source):
        if phase == 0:
            return stage.at[0:4, :, cols(peer_head)], got_kv.at[:, at(source), :]
        return stage.at[4, :, cols(peer_head)], got_q.at[at(lax.rem(source, H)), :]

    def remote(phase, peer, source, slot):
        src, dst = views(phase, lax.rem(peer, H), source)
        return pltpu.make_async_remote_copy(
            src_ref=src, dst_ref=dst,
            send_sem=send_sem.at[phase, slot], recv_sem=recv_sem.at[phase, slot],
            device_id={"seq": peer}, device_id_type=MESH)

    def own(phase):
        src, dst = views(phase, head, me)
        return pltpu.make_async_copy(src, dst, own_sem.at[phase])

    loads[4].wait()
    each(H, lambda k: remote(1, base + flipped(head, k, H), me, k).start())
    own(1).start()
    for i in range(4):
        loads[i].wait()
    each(n, lambda k: remote(0, flipped(me, k, n), me, k).start())
    own(0).start()

    ends, total = [], 0
    for p in range(sizes_ref.shape[0] - 1):
        total = total + sizes_ref[p]
        ends.append(total)

    block = 4 * rows
    scale = hd ** (-0.5)
    contract = (((1,), (1,)), ((), ()))

    def attend(b):
        at_b = pl.ds(pl.multiple_of(b * block, block), block)
        token = base * rows + b * block + lax.broadcasted_iota(jnp.int32, (block, 1), 0)
        limit = jnp.full((block, 1), keys, jnp.int32)
        for e in reversed(ends):
            limit = jnp.where(token < e, e, limit)
        fresh = lax.broadcasted_iota(jnp.int32, (block, keys), 1) < limit
        qb = got_q[at_b, :]
        sf = lax.dot_general(qb, got_kv[0], contract, preferred_element_type=jnp.float32)
        ss = lax.dot_general(qb, got_kv[1], contract, preferred_element_type=jnp.float32)
        s = jnp.where(fresh, sf, ss)
        w = jnp.exp((s - jnp.max(s, axis=1, keepdims=True)) * scale)
        den = jnp.sum(w, axis=1, keepdims=True)
        zero = jnp.zeros_like(w)
        wf = jnp.where(fresh, w, zero).astype(jnp.bfloat16)
        ws = jnp.where(fresh, zero, w).astype(jnp.bfloat16)
        num = jnp.dot(wf, got_kv[2], preferred_element_type=jnp.float32)
        num = num + jnp.dot(ws, got_kv[3], preferred_element_type=jnp.float32)
        att[at_b, :] = (num / den).astype(jnp.bfloat16)

    def back(slot):
        j = flipped(head, slot, H)
        return pltpu.make_async_remote_copy(
            src_ref=att.at[at(j), :], dst_ref=out_ref.at[:, cols(head)],
            send_sem=back_send.at[slot], recv_sem=back_recv.at[slot],
            device_id={"seq": base + j}, device_id_type=MESH)

    back_own = pltpu.make_async_copy(att.at[at(head), :], out_ref.at[:, cols(head)], own_sem.at[2])

    each(n, lambda k: remote(0, me, me, k).wait_recv())
    own(0).wait()
    for k in (2, 3, 1, 0):
        for slot in range(4 * k, 4 * k + 4):
            if slot:
                remote(1, me, me, slot).wait_recv()
            else:
                own(1).wait()
        attend(flipped(head // 4, k, H // 4))
        for slot in range(4 * k, 4 * k + 4):
            if slot:
                back(slot).start()
            else:
                back_own.start()

    each(n, lambda k: remote(0, me, me, k).wait_send())
    each(H, lambda k: remote(1, me, me, k).wait_send())
    for slot in range(1, H):
        back(slot).wait()
    back_own.wait()


def spread_shards(queries, fresh_keys, fresh_values, stale_keys, stale_values, patch_sizes):
    rows, columns = queries.shape
    n = lax.axis_size("seq")
    hd = columns // H
    keys, count = n * rows, H * rows
    dma = pltpu.SemaphoreType.DMA
    any_spec = pl.BlockSpec(memory_space=pl.ANY)
    return pl.pallas_call(
        functools.partial(spread_kernel, n),
        out_shape=pltpu.VMEM((rows, columns), queries.dtype),
        in_specs=[any_spec] * 5 + [pl.BlockSpec(memory_space=pltpu.SMEM)],
        out_specs=pl.BlockSpec(memory_space=pltpu.VMEM),
        scratch_shapes=[
            pltpu.VMEM((5, rows, columns), queries.dtype),
            pltpu.VMEM((count, hd), queries.dtype),
            pltpu.VMEM((4, keys, hd), queries.dtype),
            pltpu.VMEM((count, hd), queries.dtype),
            dma((5,)), dma((3,)), dma((2, n)), dma((2, n)), dma((H,)), dma((H,)),
        ],
        compiler_params=pltpu.CompilerParams(collective_id=0, has_side_effects=True),
    )(fresh_keys, stale_keys, fresh_values, stale_values, queries, patch_sizes)


def kernel(
    n, fk_ref, sk_ref, fv_ref, sv_ref, q_ref, sizes_hbm, out_ref,
    stage, got_q, got_kv, turned, att, lse_out, part, lse_in, mix, sizes_ref,
    load_sem, kv_recv, q_recv, o_recv, l_recv, kv_send, q_send, o_send, l_send, ready,
):
    rows, columns = q_ref.shape
    hd = columns // H
    me = lax.axis_index("seq")
    half = n // 2
    held = H // half
    keys = half * rows
    lanes = lse_in.shape[2]
    per = lanes // rows
    chips = n // 2

    for i, ref in enumerate((fk_ref, sk_ref, fv_ref, sv_ref, q_ref)):
        for r in range(0, rows, 16):
            piece = pl.ds(r, min(16, rows))
            pltpu.make_async_copy(ref.at[piece, :], stage.at[i, piece, :], load_sem.at[i // 4]).start()
    load_sizes = pltpu.make_async_copy(sizes_hbm, sizes_ref, load_sem.at[2])
    load_sizes.start()

    def signal(sem, peer):
        pl.semaphore_signal(sem, inc=1, device_id={"seq": peer}, device_id_type=MESH)

    chip = lax.div(me, 2)
    core = me - 2 * chip
    side = lax.div(me, half)
    place = chip - side * (chips // 2)
    upper = lax.rem(chip, 2) == 1
    buddy = 2 * chip + 1 - core

    floor = lax.div(chip, 2)
    barrier = pltpu.get_barrier_semaphore()
    signal(barrier, buddy)

    def tell(sem, target):
        signal(sem, 2 * target)
        signal(sem, 2 * target + 1)

    for t in range(1, chips):
        later = floor < t // 2
        if t % 2:
            pl.when(later | ((chip < t) & jnp.logical_not(upper)))(functools.partial(tell, barrier, t))
        else:
            pl.when(later & jnp.logical_not(upper))(functools.partial(tell, barrier, t))
    pl.semaphore_wait(barrier, jnp.where(upper, 4 * floor + 3, 2 * floor + 1))
    for t in range(chips - 2, -1, -1):
        if t % 2:
            pl.when((core == 1) & (chip > t) & upper)(functools.partial(tell, ready.at[chip], t))
        else:
            pl.when((core == 1) & ((floor > t // 2) | ((chip > t) & upper)))(functools.partial(tell, ready.at[chip], t))

    def cols(h, count=1):
        return pl.ds(pl.multiple_of(h * hd, hd), count * hd)

    def at(p, count=1):
        return pl.ds(pl.multiple_of(p * rows, rows), count * rows)

    def to(peer, src, dst, send, recv):
        return pltpu.make_async_remote_copy(
            src_ref=src, dst_ref=dst, send_sem=send, recv_sem=recv,
            device_id={"seq": peer}, device_id_type=MESH)

    local = me - side * half

    def kv_views(a, peer):
        return (stage.at[0:4, :, cols((peer - side * half) * held + a)], got_kv.at[a, :, at(local), :])

    def q_views(peer, base):
        return stage.at[4, :, cols((peer - base) * held, held)], got_q.at[at(me), :]

    def o_views(a, peer):
        return att.at[at(peer), a * hd:(a + 1) * hd], part.at[side, :, cols(local * held + a)]

    def l_views(peer):
        return lse_out.at[peer // per if isinstance(peer, int) else lax.div(peer, per)], lse_in.at[me]

    def send_kv(a, peer):
        to(peer, *kv_views(a, peer), kv_send.at[0], kv_recv.at[a]).start()

    def send_q(base, peer):
        to(peer, *q_views(peer, base), q_send.at[0], q_recv.at[lax.div(me, per)]).start()

    def send_o(a, peer):
        to(peer, *o_views(a, peer), o_send.at[0], o_recv.at[a]).start()

    def send_l(peer):
        to(peer, *l_views(peer), l_send.at[0], l_recv.at[0]).start()

    def arrived(sem, ref):
        to(me, ref, ref, sem, sem).wait_recv()

    def left(sem, ref):
        to(me, ref, ref, sem, sem).wait_send()

    def keep(src, dst):
        dst[...] = src[...]

    def cores(target, body):
        body(2 * target)
        body(2 * target + 1)

    def hear(target):
        pl.semaphore_wait(ready.at[target], 1)

    quad = chips // 2

    first = side * quad
    across = 2 * first + quad - 1 - chip
    along = first + lax.rem(place + 2, quad)
    beside = chip + 1 - 2 * lax.rem(chip, 2)

    def nears(body):
        swap = place == 1
        for target in (jnp.where(swap, along, across), jnp.where(swap, across, along), beside):
            cores(target, body)

    arrived(load_sem.at[0], stage.at[0:4])
    head_a = functools.partial(send_kv, 0)
    head_a(buddy)

    @pl.when(place == 0)
    def _():
        for target in (beside, along, across):
            hear(target)
            cores(target, head_a)

    @pl.when(place == 1)
    def _():
        cores(beside, head_a)
        hear(along)
        cores(across, head_a)
        cores(along, head_a)

    @pl.when(place == 2)
    def _():
        cores(along, head_a)
        hear(beside)
        cores(across, head_a)
        cores(beside, head_a)

    @pl.when(place == 3)
    def _():
        nears(head_a)

    arrived(load_sem.at[1], stage.at[4])

    last_plane = n // per - 1

    def send_one(a, peer):
        src = stage.at[4, :, cols(peer * held + a)]
        dst = got_q.at[at(me), a * hd:(a + 1) * hd]
        to(peer, src, dst, q_send.at[0], q_recv.at[last_plane + a]).start()

    @pl.when((side == 1) & (place < 2))
    def _():
        for t in range(quad):
            cores(t, functools.partial(send_q, 0))

    def send_low(a):
        for t in range(quad):
            cores(t, functools.partial(send_one, a))

    pl.when((side == 1) & (place >= 2))(functools.partial(send_low, 0))

    @pl.when(side == 0)
    def _():
        far = functools.partial(send_q, half)
        for t in range(quad, chips, 2):
            now = place < (2 if t + 2 == chips else quad)

            @pl.when(jnp.logical_not(upper))
            def _():
                hear(t)
                pl.when(now)(lambda: cores(t, far))
                hear(t + 1)
                pl.when(now)(lambda: cores(t + 1, far))

            @pl.when(upper)
            def _():
                hear(t + 1)

                @pl.when(now)
                def _():
                    cores(t + 1, far)
                    cores(t, far)

    def send_top_q():
        for t in (chips - 2, chips - 1):
            cores(t, functools.partial(send_q, half))

    def send_near_q():
        near_q = functools.partial(send_q, side * half)
        near_q(buddy)
        nears(near_q)

    pl.when(side == 0)(send_near_q)
    for a in range(1, held):
        send_kv(a, buddy)
        nears(functools.partial(send_kv, a))
    for a in range(1, held):
        pl.when((side == 1) & (place >= 2))(functools.partial(send_low, a))
    pl.when(side == 1)(send_near_q)
    for a in range(held):
        keep(*kv_views(a, me))
    keep(*q_views(me, side * half))
    load_sizes.wait()

    ends, total = [], 0
    for p in range(sizes_ref.shape[0] - 1):
        total = total + sizes_ref[p]
        ends.append(total)

    scale = hd ** (-0.5) * 1.4426950408889634
    contract = (((1,), (1,)), ((), ()))

    def turn(a):
        turned[a, :, 0:keys] = got_kv[a, 2].T
        turned[a, :, keys:2 * keys] = got_kv[a, 3].T

    def attend(a, start, count):
        at_q = slice(start, start + count)
        token = start + lax.broadcasted_iota(jnp.int32, (1, count), 1)
        limit = jnp.full((1, count), 2 * keys, jnp.int32)
        for e in reversed(ends):
            limit = jnp.where(token < e, e, limit)
        fresh = lax.broadcasted_iota(jnp.int32, (keys, count), 0) < limit - side * keys
        both = got_kv[a, 0:2].reshape(2 * keys, hd)
        qb = got_q[at_q, a * hd:(a + 1) * hd]
        x = lax.dot_general(both, qb, contract, preferred_element_type=jnp.float32)
        x = jnp.where(fresh, x[:keys], x[keys:])
        top = jnp.max(x, axis=0, keepdims=True)
        w = jnp.exp2((x - top) * scale)
        den = jnp.sum(w, axis=0, keepdims=True)
        zero = jnp.zeros_like(w)
        wf = jnp.where(fresh, w, zero).astype(jnp.bfloat16)
        ws = jnp.where(fresh, zero, w).astype(jnp.bfloat16)
        num = jnp.dot(turned[a], jnp.concatenate([wf, ws], axis=0), preferred_element_type=jnp.float32)
        att[at_q, a * hd:(a + 1) * hd] = (num * (1.0 / den)).T.astype(jnp.bfloat16)
        lse = top * scale + jnp.log2(den)
        for b in range(count // lanes):
            lse_out[start // lanes + b, a:a + 1, :] = lse[:, b * lanes:(b + 1) * lanes]

    def give(a, planes, last):
        for p in planes if planes[0] < n // per // 2 else reversed(planes):
            for j in range(p * per, (p + 1) * per):
                @pl.when(me != j)
                def _(j=j):
                    if last:
                        send_l(j)
                    send_o(a, j)

    def own(a, last):
        if last:
            keep(*l_views(me))
        keep(*o_views(a, me))

    def work(a, planes, mine, last=False):
        attend(a, planes[0] * lanes, len(planes) * lanes)
        give(a, planes, last)
        if mine:
            own(a, last)

    def wait_kv(a):
        arrived(kv_recv.at[a], got_kv.at[a, :, 0:(half - 1) * rows, :])
        turn(a)

    def wait_q(planes, mine):
        for p in planes:
            if mine:
                pl.when(lax.div(me, per) == p)(lambda p=p: arrived(q_recv.at[p], got_q.at[0:(per - 1) * rows, :]))
                pl.when(lax.div(me, per) != p)(lambda p=p: arrived(q_recv.at[p], got_q.at[0:per * rows, :]))
            else:
                arrived(q_recv.at[p], got_q.at[0:per * rows, :])

    def wait_one(a):
        arrived(q_recv.at[last_plane + a], got_q.at[0:per * rows, 0:hd])

    planes = n // per
    low_planes, high_planes = range(planes // 2), range(planes // 2, planes)
    end = held - 1

    @pl.when(side == 0)
    def _():
        wait_kv(0)
        pl.when(place >= 2)(send_top_q)
        wait_q(high_planes[:1], False)
        work(0, high_planes[:1], False)
        wait_q(low_planes, True)
        work(0, low_planes, True)
        last = high_planes[-1:]
        wait_one(0)
        work(0, last, False)
        for a in range(1, held):
            wait_kv(a)
            work(a, low_planes, True, a == end)
            wait_one(a)
            work(a, high_planes, False, a == end)

    @pl.when(side == 1)
    def _():
        @pl.when(place < 2)
        def _():
            for a in range(held):
                wait_kv(a)
                if a == 0:
                    wait_q(low_planes, False)
                work(a, low_planes, False, a == end)

        @pl.when(place >= 2)
        def _():
            for p in low_planes:
                for a in range(held):
                    if p == 0:
                        wait_kv(a)
                    if a == 0:
                        wait_q([p], False)
                    work(a, [p], False, a == end)

        wait_q(high_planes, True)
        for a in range(held):
            work(a, high_planes, True, a == end)

    most = (n - 1) * rows
    arrived(l_recv.at[0], lse_in.at[0:n - 1])
    low = lse_in[0:half].reshape(H, lanes)
    high = lse_in[half:n].reshape(H, lanes)
    top = jnp.maximum(low, high)
    low, high = jnp.exp2(low - top), jnp.exp2(high - top)
    total = low + high
    fill = jnp.zeros((lanes - 2 * H, lanes), jnp.float32)
    mix[...] = jnp.concatenate([low / total, high / total, fill], axis=0).T
    share = mix[at(lax.rem(me, per)), :]
    for a in range(held):
        arrived(o_recv.at[a], att.at[0:most, 0:hd])
        for h in range(a, H, held):
            c = slice(h * hd, (h + 1) * hd)
            out = share[:, h:h + 1] * part[0, :, c].astype(jnp.float32)
            out = out + share[:, H + h:H + h + 1] * part[1, :, c].astype(jnp.float32)
            out_ref[:, c] = out.astype(out_ref.dtype)

    left(kv_send.at[0], got_kv.at[:, :, 0:(half - 1) * rows, :])
    left(q_send.at[0], got_q.at[0:most, :])
    left(o_send.at[0], att.at[0:most, :])
    left(l_send.at[0], lse_in.at[0:n - 1])


def shards(queries, fresh_keys, fresh_values, stale_keys, stale_values, patch_sizes):
    rows, columns = queries.shape
    n = lax.axis_size("seq")
    hd = columns // H
    half = n // 2
    held = H // half
    keys, lanes = half * rows, 128
    dma = pltpu.SemaphoreType.DMA
    kind = queries.dtype
    return pl.pallas_call(
        functools.partial(kernel, n),
        out_shape=pltpu.VMEM((rows, columns), kind),
        in_specs=[pl.BlockSpec(memory_space=pl.ANY)] * 6,
        out_specs=pl.BlockSpec(memory_space=pltpu.VMEM),
        scratch_shapes=[
            pltpu.VMEM((5, rows, columns), kind),
            pltpu.VMEM((n * rows, held * hd), kind),
            pltpu.VMEM((held, 4, keys, hd), kind),
            pltpu.VMEM((held, hd, 2 * keys), kind),
            pltpu.VMEM((n * rows, held * hd), kind),
            pltpu.VMEM((n * rows // lanes, held, lanes), jnp.float32),
            pltpu.VMEM((2, rows, columns), kind),
            pltpu.VMEM((n, held, lanes), jnp.float32),
            pltpu.VMEM((lanes, lanes), jnp.float32),
            pltpu.SMEM(patch_sizes.shape, patch_sizes.dtype),
            dma((3,)), dma((held,)), dma((n * rows // lanes + held - 1,)), dma((held,)), dma((1,)),
            dma((1,)), dma((1,)), dma((1,)), dma((1,)),
            pltpu.SemaphoreType.REGULAR((n // 2,)),
        ],
        compiler_params=pltpu.CompilerParams(collective_id=0, has_side_effects=True),
    )(fresh_keys, stale_keys, fresh_values, stale_values, queries, patch_sizes)


def solution(mesh):
    spec = P(("groups", "seq"), None)
    body = shards if mesh.shape["seq"] == H else spread_shards
    return jax.shard_map(
        body, mesh=mesh, in_specs=(spec,) * 5 + (P("groups"),), out_specs=spec, check_vma=False)
```

```python
import functools

import jax
import jax.numpy as jnp
from jax import lax
from jax.experimental import pallas as pl
from jax.experimental.pallas import tpu as pltpu
from jax.sharding import PartitionSpec as P

H = 16
MESH = pl.DeviceIdType.MESH


def each(count, body):
    if count <= 32:
        for k in range(1, count):
            body(k)
    else:
        lax.fori_loop(1, count, lambda k, c: (body(k), c)[1], 0)


def flipped(me, k, count):
    if count & (count - 1):
        return lax.rem(me + k, count)
    peer, bit = 0, 1
    while bit < count:
        peer = peer + bit * lax.rem(me // bit + k // bit, 2)
        bit *= 2
    return peer


def spread_kernel(
    n, fk_ref, sk_ref, fv_ref, sv_ref, q_ref, sizes_ref, out_ref,
    stage, got_q, got_kv, att,
    load_sem, own_sem, send_sem, recv_sem, back_send, back_recv,
):
    rows, columns = q_ref.shape
    hd = columns // H
    me = lax.axis_index("seq")
    head = lax.rem(me, H)
    base = me - head
    keys = n * rows
    queries = H * rows

    loads = []
    for i, ref in enumerate((fk_ref, sk_ref, fv_ref, sv_ref, q_ref)):
        c = pltpu.make_async_copy(ref, stage.at[i], load_sem.at[i])
        c.start()
        loads.append(c)

    barrier = pltpu.get_barrier_semaphore()
    each(n, lambda k: pl.semaphore_signal(
        barrier, inc=1, device_id={"seq": flipped(me, k, n)}, device_id_type=MESH))
    pl.semaphore_wait(barrier, n - 1)

    def cols(h):
        return pl.ds(pl.multiple_of(h * hd, hd), hd)

    def at(p):
        return pl.ds(pl.multiple_of(p * rows, rows), rows)

    def views(phase, peer_head, source):
        if phase == 0:
            return stage.at[0:4, :, cols(peer_head)], got_kv.at[:, at(source), :]
        return stage.at[4, :, cols(peer_head)], got_q.at[at(lax.rem(source, H)), :]

    def remote(phase, peer, source, slot):
        src, dst = views(phase, lax.rem(peer, H), source)
        return pltpu.make_async_remote_copy(
            src_ref=src, dst_ref=dst,
            send_sem=send_sem.at[phase, slot], recv_sem=recv_sem.at[phase, slot],
            device_id={"seq": peer}, device_id_type=MESH)

    def own(phase):
        src, dst = views(phase, head, me)
        return pltpu.make_async_copy(src, dst, own_sem.at[phase])

    loads[4].wait()
    each(H, lambda k: remote(1, base + flipped(head, k, H), me, k).start())
    own(1).start()
    for i in range(4):
        loads[i].wait()
    each(n, lambda k: remote(0, flipped(me, k, n), me, k).start())
    own(0).start()

    ends, total = [], 0
    for p in range(sizes_ref.shape[0] - 1):
        total = total + sizes_ref[p]
        ends.append(total)

    block = 4 * rows
    scale = hd ** (-0.5)
    contract = (((1,), (1,)), ((), ()))

    def attend(b):
        at_b = pl.ds(pl.multiple_of(b * block, block), block)
        token = base * rows + b * block + lax.broadcasted_iota(jnp.int32, (block, 1), 0)
        limit = jnp.full((block, 1), keys, jnp.int32)
        for e in reversed(ends):
            limit = jnp.where(token < e, e, limit)
        fresh = lax.broadcasted_iota(jnp.int32, (block, keys), 1) < limit
        qb = got_q[at_b, :]
        sf = lax.dot_general(qb, got_kv[0], contract, preferred_element_type=jnp.float32)
        ss = lax.dot_general(qb, got_kv[1], contract, preferred_element_type=jnp.float32)
        s = jnp.where(fresh, sf, ss)
        w = jnp.exp((s - jnp.max(s, axis=1, keepdims=True)) * scale)
        den = jnp.sum(w, axis=1, keepdims=True)
        zero = jnp.zeros_like(w)
        wf = jnp.where(fresh, w, zero).astype(jnp.bfloat16)
        ws = jnp.where(fresh, zero, w).astype(jnp.bfloat16)
        num = jnp.dot(wf, got_kv[2], preferred_element_type=jnp.float32)
        num = num + jnp.dot(ws, got_kv[3], preferred_element_type=jnp.float32)
        att[at_b, :] = (num / den).astype(jnp.bfloat16)

    def back(slot):
        j = flipped(head, slot, H)
        return pltpu.make_async_remote_copy(
            src_ref=att.at[at(j), :], dst_ref=out_ref.at[:, cols(head)],
            send_sem=back_send.at[slot], recv_sem=back_recv.at[slot],
            device_id={"seq": base + j}, device_id_type=MESH)

    back_own = pltpu.make_async_copy(att.at[at(head), :], out_ref.at[:, cols(head)], own_sem.at[2])

    each(n, lambda k: remote(0, me, me, k).wait_recv())
    own(0).wait()
    for k in (2, 3, 1, 0):
        for slot in range(4 * k, 4 * k + 4):
            if slot:
                remote(1, me, me, slot).wait_recv()
            else:
                own(1).wait()
        attend(flipped(head // 4, k, H // 4))
        for slot in range(4 * k, 4 * k + 4):
            if slot:
                back(slot).start()
            else:
                back_own.start()

    each(n, lambda k: remote(0, me, me, k).wait_send())
    each(H, lambda k: remote(1, me, me, k).wait_send())
    for slot in range(1, H):
        back(slot).wait()
    back_own.wait()


def spread_shards(queries, fresh_keys, fresh_values, stale_keys, stale_values, patch_sizes):
    rows, columns = queries.shape
    n = lax.axis_size("seq")
    hd = columns // H
    keys, count = n * rows, H * rows
    dma = pltpu.SemaphoreType.DMA
    any_spec = pl.BlockSpec(memory_space=pl.ANY)
    return pl.pallas_call(
        functools.partial(spread_kernel, n),
        out_shape=pltpu.VMEM((rows, columns), queries.dtype),
        in_specs=[any_spec] * 5 + [pl.BlockSpec(memory_space=pltpu.SMEM)],
        out_specs=pl.BlockSpec(memory_space=pltpu.VMEM),
        scratch_shapes=[
            pltpu.VMEM((5, rows, columns), queries.dtype),
            pltpu.VMEM((count, hd), queries.dtype),
            pltpu.VMEM((4, keys, hd), queries.dtype),
            pltpu.VMEM((count, hd), queries.dtype),
            dma((5,)), dma((3,)), dma((2, n)), dma((2, n)), dma((H,)), dma((H,)),
        ],
        compiler_params=pltpu.CompilerParams(collective_id=0, has_side_effects=True),
    )(fresh_keys, stale_keys, fresh_values, stale_values, queries, patch_sizes)


def kernel(
    n, fk_ref, sk_ref, fv_ref, sv_ref, q_ref, sizes_hbm, out_ref,
    stage, got_q, got_kv, turned, att, lse_out, part, lse_in, mix, sizes_ref,
    load_sem, kv_recv, q_recv, o_recv, l_recv, kv_send, q_send, o_send, l_send, ready,
):
    rows, columns = q_ref.shape
    hd = columns // H
    me = lax.axis_index("seq")
    half = n // 2
    held = H // half
    keys = half * rows
    lanes = lse_in.shape[2]
    per = lanes // rows
    chips = n // 2

    for i, ref in enumerate((fk_ref, sk_ref, fv_ref, sv_ref, q_ref)):
        for r in range(0, rows, 16):
            piece = pl.ds(r, min(16, rows))
            pltpu.make_async_copy(ref.at[piece, :], stage.at[i, piece, :], load_sem.at[i // 4]).start()
    load_sizes = pltpu.make_async_copy(sizes_hbm, sizes_ref, load_sem.at[2])
    load_sizes.start()

    def signal(sem, peer):
        pl.semaphore_signal(sem, inc=1, device_id={"seq": peer}, device_id_type=MESH)

    chip = lax.div(me, 2)
    core = me - 2 * chip
    side = lax.div(me, half)
    place = chip - side * (chips // 2)
    upper = lax.rem(chip, 2) == 1
    buddy = 2 * chip + 1 - core

    floor = lax.div(chip, 2)
    barrier = pltpu.get_barrier_semaphore()
    signal(barrier, buddy)

    def tell(sem, target):
        signal(sem, 2 * target)
        signal(sem, 2 * target + 1)

    for t in range(1, chips):
        later = floor < t // 2
        if t % 2:
            pl.when(later | ((chip < t) & jnp.logical_not(upper)))(functools.partial(tell, barrier, t))
        else:
            pl.when(later & jnp.logical_not(upper))(functools.partial(tell, barrier, t))
    pl.semaphore_wait(barrier, jnp.where(upper, 4 * floor + 3, 2 * floor + 1))
    for t in range(chips - 2, -1, -1):
        if t % 2:
            pl.when((core == 1) & (chip > t) & upper)(functools.partial(tell, ready.at[chip], t))
        else:
            pl.when((core == 1) & ((floor > t // 2) | ((chip > t) & upper)))(functools.partial(tell, ready.at[chip], t))

    def cols(h, count=1):
        return pl.ds(pl.multiple_of(h * hd, hd), count * hd)

    def at(p, count=1):
        return pl.ds(pl.multiple_of(p * rows, rows), count * rows)

    def to(peer, src, dst, send, recv):
        return pltpu.make_async_remote_copy(
            src_ref=src, dst_ref=dst, send_sem=send, recv_sem=recv,
            device_id={"seq": peer}, device_id_type=MESH)

    local = me - side * half

    def kv_views(a, peer):
        return (stage.at[0:4, :, cols((peer - side * half) * held + a)], got_kv.at[a, :, at(local), :])

    def q_views(peer, base):
        return stage.at[4, :, cols((peer - base) * held, held)], got_q.at[at(me), :]

    def o_views(a, peer):
        return att.at[at(peer), a * hd:(a + 1) * hd], part.at[side, :, cols(local * held + a)]

    def l_views(peer):
        return lse_out.at[peer // per if isinstance(peer, int) else lax.div(peer, per)], lse_in.at[me]

    def send_kv(a, peer):
        to(peer, *kv_views(a, peer), kv_send.at[0], kv_recv.at[a]).start()

    def send_q(base, peer):
        to(peer, *q_views(peer, base), q_send.at[0], q_recv.at[lax.div(me, per)]).start()

    def send_o(a, peer):
        to(peer, *o_views(a, peer), o_send.at[0], o_recv.at[a]).start()

    def send_l(peer):
        to(peer, *l_views(peer), l_send.at[0], l_recv.at[0]).start()

    def arrived(sem, ref):
        to(me, ref, ref, sem, sem).wait_recv()

    def left(sem, ref):
        to(me, ref, ref, sem, sem).wait_send()

    def keep(src, dst):
        dst[...] = src[...]

    def cores(target, body):
        body(2 * target)
        body(2 * target + 1)

    def hear(target):
        pl.semaphore_wait(ready.at[target], 1)

    quad = chips // 2

    first = side * quad
    across = 2 * first + quad - 1 - chip
    along = first + lax.rem(place + 2, quad)
    beside = chip + 1 - 2 * lax.rem(chip, 2)

    def nears(body):
        swap = place == 1
        for target in (jnp.where(swap, along, across), jnp.where(swap, across, along), beside):
            cores(target, body)

    arrived(load_sem.at[0], stage.at[0:4])
    head_a = functools.partial(send_kv, 0)
    head_a(buddy)

    @pl.when(place == 0)
    def _():
        for target in (beside, along, across):
            hear(target)
            cores(target, head_a)

    @pl.when(place == 1)
    def _():
        cores(beside, head_a)
        hear(along)
        cores(across, head_a)
        cores(along, head_a)

    @pl.when(place == 2)
    def _():
        cores(along, head_a)
        hear(beside)
        cores(across, head_a)
        cores(beside, head_a)

    @pl.when(place == 3)
    def _():
        nears(head_a)

    arrived(load_sem.at[1], stage.at[4])

    last_plane = n // per - 1

    def send_one(a, peer):
        src = stage.at[4, :, cols(peer * held + a)]
        dst = got_q.at[at(me), a * hd:(a + 1) * hd]
        to(peer, src, dst, q_send.at[0], q_recv.at[last_plane + a]).start()

    @pl.when((side == 1) & (place < 2))
    def _():
        for t in range(quad):
            cores(t, functools.partial(send_q, 0))

    def send_low(a):
        for t in range(quad):
            cores(t, functools.partial(send_one, a))

    pl.when((side == 1) & (place >= 2))(functools.partial(send_low, 0))

    @pl.when(side == 0)
    def _():
        far = functools.partial(send_q, half)
        for t in range(quad, chips, 2):
            now = place < (2 if t + 2 == chips else quad)

            @pl.when(jnp.logical_not(upper))
            def _():
                hear(t)
                pl.when(now)(lambda: cores(t, far))
                hear(t + 1)
                pl.when(now)(lambda: cores(t + 1, far))

            @pl.when(upper)
            def _():
                hear(t + 1)

                @pl.when(now)
                def _():
                    cores(t + 1, far)
                    cores(t, far)

    def send_top_q():
        for t in (chips - 2, chips - 1):
            cores(t, functools.partial(send_q, half))

    def send_near_q():
        near_q = functools.partial(send_q, side * half)
        near_q(buddy)
        nears(near_q)

    pl.when(side == 0)(send_near_q)
    for a in range(1, held):
        send_kv(a, buddy)
        nears(functools.partial(send_kv, a))
    for a in range(1, held):
        pl.when((side == 1) & (place >= 2))(functools.partial(send_low, a))
    pl.when(side == 1)(send_near_q)
    for a in range(held):
        keep(*kv_views(a, me))
    keep(*q_views(me, side * half))
    load_sizes.wait()

    ends, total = [], 0
    for p in range(sizes_ref.shape[0] - 1):
        total = total + sizes_ref[p]
        ends.append(total)

    scale = hd ** (-0.5) * 1.4426950408889634
    contract = (((1,), (1,)), ((), ()))

    def turn(a):
        turned[a, :, 0:keys] = got_kv[a, 2].T
        turned[a, :, keys:2 * keys] = got_kv[a, 3].T

    def attend(a, start, count):
        at_q = slice(start, start + count)
        token = start + lax.broadcasted_iota(jnp.int32, (1, count), 1)
        limit = jnp.full((1, count), 2 * keys, jnp.int32)
        for e in reversed(ends):
            limit = jnp.where(token < e, e, limit)
        fresh = lax.broadcasted_iota(jnp.int32, (keys, count), 0) < limit - side * keys
        both = got_kv[a, 0:2].reshape(2 * keys, hd)
        qb = got_q[at_q, a * hd:(a + 1) * hd]
        x = lax.dot_general(both, qb, contract, preferred_element_type=jnp.float32)
        x = jnp.where(fresh, x[:keys], x[keys:])
        top = jnp.max(x, axis=0, keepdims=True)
        w = jnp.exp2((x - top) * scale)
        den = jnp.sum(w, axis=0, keepdims=True)
        zero = jnp.zeros_like(w)
        wf = jnp.where(fresh, w, zero).astype(jnp.bfloat16)
        ws = jnp.where(fresh, zero, w).astype(jnp.bfloat16)
        num = jnp.dot(turned[a], jnp.concatenate([wf, ws], axis=0), preferred_element_type=jnp.float32)
        att[at_q, a * hd:(a + 1) * hd] = (num * (1.0 / den)).T.astype(jnp.bfloat16)
        lse = top * scale + jnp.log2(den)
        for b in range(count // lanes):
            lse_out[start // lanes + b, a:a + 1, :] = lse[:, b * lanes:(b + 1) * lanes]

    def give(a, planes, last, turned_round):
        for p in reversed(planes) if turned_round else planes:
            for j in range(p * per, (p + 1) * per):
                @pl.when(me != j)
                def _(j=j):
                    if last:
                        send_l(j)
                    send_o(a, j)

    def own(a, last):
        if last:
            keep(*l_views(me))
        keep(*o_views(a, me))

    def work(a, planes, mine, last=False):
        attend(a, planes[0] * lanes, len(planes) * lanes)
        give(a, planes, last, not mine and planes[0] > 0)
        if mine:
            own(a, last)

    def wait_kv(a):
        arrived(kv_recv.at[a], got_kv.at[a, :, 0:(half - 1) * rows, :])
        turn(a)

    def wait_q(planes, mine):
        for p in planes:
            if mine:
                pl.when(lax.div(me, per) == p)(lambda p=p: arrived(q_recv.at[p], got_q.at[0:(per - 1) * rows, :]))
                pl.when(lax.div(me, per) != p)(lambda p=p: arrived(q_recv.at[p], got_q.at[0:per * rows, :]))
            else:
                arrived(q_recv.at[p], got_q.at[0:per * rows, :])

    def wait_one(a):
        arrived(q_recv.at[last_plane + a], got_q.at[0:per * rows, 0:hd])

    planes = n // per
    low_planes, high_planes = range(planes // 2), range(planes // 2, planes)
    end = held - 1

    @pl.when(side == 0)
    def _():
        wait_kv(0)
        pl.when(place >= 2)(send_top_q)
        wait_q(high_planes[:1], False)
        work(0, high_planes[:1], False)
        wait_q(low_planes, True)
        work(0, low_planes, True)
        last = high_planes[-1:]
        wait_one(0)
        work(0, last, False)
        for a in range(1, held):
            wait_kv(a)
            work(a, low_planes, True, a == end)
            wait_one(a)
            work(a, high_planes, False, a == end)

    @pl.when(side == 1)
    def _():
        @pl.when(place < 2)
        def _():
            for a in range(held):
                wait_kv(a)
                if a == 0:
                    wait_q(low_planes, False)
                work(a, low_planes, False, a == end)

        @pl.when(place >= 2)
        def _():
            for p in low_planes:
                for a in range(held):
                    if p == 0:
                        wait_kv(a)
                    if a == 0:
                        wait_q([p], False)
                    work(a, [p], False, a == end)

        wait_q(high_planes, True)
        for a in range(held):
            work(a, high_planes, True, a == end)

    most = (n - 1) * rows
    arrived(l_recv.at[0], lse_in.at[0:n - 1])
    low = lse_in[0:half].reshape(H, lanes)
    high = lse_in[half:n].reshape(H, lanes)
    top = jnp.maximum(low, high)
    low, high = jnp.exp2(low - top), jnp.exp2(high - top)
    total = low + high
    fill = jnp.zeros((lanes - 2 * H, lanes), jnp.float32)
    mix[...] = jnp.concatenate([low / total, high / total, fill], axis=0).T
    share = mix[at(lax.rem(me, per)), :]
    for a in range(held):
        arrived(o_recv.at[a], att.at[0:most, 0:hd])
        for h in range(a, H, held):
            c = slice(h * hd, (h + 1) * hd)
            out = share[:, h:h + 1] * part[0, :, c].astype(jnp.float32)
            out = out + share[:, H + h:H + h + 1] * part[1, :, c].astype(jnp.float32)
            out_ref[:, c] = out.astype(out_ref.dtype)

    left(kv_send.at[0], got_kv.at[:, :, 0:(half - 1) * rows, :])
    left(q_send.at[0], got_q.at[0:most, :])
    left(o_send.at[0], att.at[0:most, :])
    left(l_send.at[0], lse_in.at[0:n - 1])


def shards(queries, fresh_keys, fresh_values, stale_keys, stale_values, patch_sizes):
    rows, columns = queries.shape
    n = lax.axis_size("seq")
    hd = columns // H
    half = n // 2
    held = H // half
    keys, lanes = half * rows, 128
    dma = pltpu.SemaphoreType.DMA
    kind = queries.dtype
    return pl.pallas_call(
        functools.partial(kernel, n),
        out_shape=pltpu.VMEM((rows, columns), kind),
        in_specs=[pl.BlockSpec(memory_space=pl.ANY)] * 6,
        out_specs=pl.BlockSpec(memory_space=pltpu.VMEM),
        scratch_shapes=[
            pltpu.VMEM((5, rows, columns), kind),
            pltpu.VMEM((n * rows, held * hd), kind),
            pltpu.VMEM((held, 4, keys, hd), kind),
            pltpu.VMEM((held, hd, 2 * keys), kind),
            pltpu.VMEM((n * rows, held * hd), kind),
            pltpu.VMEM((n * rows // lanes, held, lanes), jnp.float32),
            pltpu.VMEM((2, rows, columns), kind),
            pltpu.VMEM((n, held, lanes), jnp.float32),
            pltpu.VMEM((lanes, lanes), jnp.float32),
            pltpu.SMEM(patch_sizes.shape, patch_sizes.dtype),
            dma((3,)), dma((held,)), dma((n * rows // lanes + held - 1,)), dma((held,)), dma((1,)),
            dma((1,)), dma((1,)), dma((1,)), dma((1,)),
            pltpu.SemaphoreType.REGULAR((n // 2,)),
        ],
        compiler_params=pltpu.CompilerParams(collective_id=0, has_side_effects=True),
    )(fresh_keys, stale_keys, fresh_values, stale_values, queries, patch_sizes)


def solution(mesh):
    spec = P(("groups", "seq"), None)
    body = shards if mesh.shape["seq"] == H else spread_shards
    return jax.shard_map(
        body, mesh=mesh, in_specs=(spec,) * 5 + (P("groups"),), out_specs=spec, check_vma=False)
```
